128 devices in a mesh: tile: 64 (over x, z, y_lo, core), split: 2 (over y_hi).
Axes of the slice: x: 4, y: 4 (y_hi: 2, y_lo: 2; y = y_hi * 2 + y_lo), z: 4, core: 2. Of those that a mesh axis runs over, the one named last changes fastest.
Arguments:
- noisy_image: bfloat16 [64, 45, 128, 128], P('tile', None, 'split'), may hold values from -60 to 60
- seam_codes: int32 [64, 4], replicated, may hold values from 0 to 3
- timestep: int32 [1], replicated, may hold values from 0 to 999
- time_weight: float32 [48, 192], replicated, may hold values from -0.875 to 0.875
- bias_upper: float32 [192, 48], replicated, may hold values from -0.875 to 0.875
- bias_lower: float32 [192, 96], replicated, may hold values from -0.875 to 0.875
- kernel_upper_first: bfloat16 [3, 3, 48, 45], replicated, may hold values from -0.3125 to 0.3125
- kernel_upper_second: bfloat16 [3, 3, 48, 48], replicated, may hold values from -0.3125 to 0.3125
- kernel_lower_first: bfloat16 [3, 3, 96, 48], replicated, may hold values from -0.3125 to 0.3125
- kernel_lower_second: bfloat16 [3, 3, 96, 96], replicated, may hold values from -0.21875 to 0.21875
- kernel_decode_first: bfloat16 [3, 3, 48, 144], replicated, may hold values from -0.15625 to 0.15625
- kernel_decode_second: bfloat16 [3, 3, 48, 48], replicated, may hold values from -0.3125 to 0.3125
- output_weight: bfloat16 [45, 48], replicated, may hold values from -0.875 to 0.875
- gains_upper: float32 [4, 48], replicated, may hold values from 0.25 to 1.75
- shifts_upper: float32 [4, 48], replicated, may hold values from -1 to 1
- gains_lower: float32 [2, 96], replicated, may hold values from 0.25 to 1.75
- shifts_lower: float32 [2, 96], replicated, may hold values from -1 to 1
Outputs:
- predicted_noise: bfloat16 [64, 45, 128, 128], P('tile', None, 'split')
The draws below stay inside these ranges and needn't reach their ends.
All inputs are finite; a program needn't handle non-finite values.
Results may differ from the reference program's by a relative error of at most 0.018.
Values may be sent and summed in bfloat16 or wider, within the bound.
No kernel may reach another device: no remote copies, remote signals or barrier semaphores. Data moves between devices by JAX's collectives and lax.ppermute only.
A program may use at most 128 MiB of HBM per device.

```python
import math
import jax
import jax.numpy as jnp
from jax import lax

CHANNELS = 45
WIDTH_ONE = 48
WIDTH_TWO = 96
EMBED = 192
GROUPS = 8
ROW_TILES = 4
SIDE = 128
TILES = 64


def draw_noisy_image(key, part):
    first_key = jax.random.fold_in(jax.random.fold_in(key, 17), 0)
    places = jnp.arange(TILES, dtype=jnp.float32)
    tile_scale = 1.0 + 2.0 * places / max(TILES - 1, 1)
    shape = (TILES, CHANNELS, SIDE, SIDE)
    base = jnp.clip(jax.random.normal(first_key, shape, jnp.float32), -6.0, 6.0)
    return (base * tile_scale[:, None, None, None]).astype(jnp.bfloat16)


def plant(entries, stream_key, least, top_value):
    shape = entries.shape
    spot = [jax.random.randint(jax.random.fold_in(stream_key, axis), (), 0, shape[axis]) for axis in range(len(shape))]
    entries = entries.at[tuple(spot)].set(least)
    longest = shape.index(max(shape))
    spot[longest] = (spot[longest] + 1) % shape[longest]
    return entries.at[tuple(spot)].set(top_value)


def normal_values(own_key, shape, scale, bound, kind=jnp.bfloat16):
    result = jax.random.normal(own_key, shape, jnp.float32) * scale
    return jnp.minimum(jnp.maximum(result, -bound), bound).astype(kind)


def setup_inputs(seed: int = 0) -> dict:
    key_list = jax.random.split(jax.random.key(seed), 18)
    noisy_image = draw_noisy_image(jax.random.fold_in(key_list[17], 71), 0)
    seam_codes = plant(jax.random.randint(key_list[1], (TILES, 4), 0, 4), jax.random.fold_in(key_list[1], 1), 0, 3).astype(jnp.int32)
    timestep = jax.random.randint(key_list[2], (1,), 0, 1000).astype(jnp.int32)
    time_weight = normal_values(key_list[3], (WIDTH_ONE, EMBED), WIDTH_ONE ** -0.5, 0.875, jnp.float32)
    bias_upper = normal_values(key_list[4], (EMBED, WIDTH_ONE), (EMBED // 4) ** -0.5, 0.875, jnp.float32)
    bias_lower = normal_values(key_list[5], (EMBED, WIDTH_TWO), (EMBED // 4) ** -0.5, 0.875, jnp.float32)
    kernel_upper_first = normal_values(key_list[6], (3, 3, WIDTH_ONE, CHANNELS), (9 * CHANNELS) ** -0.5, 0.3125)
    kernel_upper_second = normal_values(key_list[7], (3, 3, WIDTH_ONE, WIDTH_ONE), (9 * WIDTH_ONE) ** -0.5, 0.3125)
    kernel_lower_first = normal_values(key_list[8], (3, 3, WIDTH_TWO, WIDTH_ONE), (9 * WIDTH_ONE) ** -0.5, 0.3125)
    kernel_lower_second = normal_values(key_list[9], (3, 3, WIDTH_TWO, WIDTH_TWO), (9 * WIDTH_TWO) ** -0.5, 0.21875)
    kernel_decode_first = normal_values(key_list[10], (3, 3, WIDTH_ONE, WIDTH_TWO + WIDTH_ONE), (9 * (WIDTH_TWO + WIDTH_ONE)) ** -0.5, 0.15625)
    kernel_decode_second = normal_values(key_list[11], (3, 3, WIDTH_ONE, WIDTH_ONE), (9 * WIDTH_ONE) ** -0.5, 0.3125)
    output_weight = normal_values(key_list[12], (CHANNELS, WIDTH_ONE), WIDTH_ONE ** -0.5, 0.875)
    gains_upper = jnp.clip(1.0 + 0.15 * jax.random.normal(key_list[13], (4, WIDTH_ONE), jnp.float32), 0.25, 1.75)
    shifts_upper = normal_values(key_list[14], (4, WIDTH_ONE), 0.3, 1.0, jnp.float32)
    gains_lower = jnp.clip(1.0 + 0.15 * jax.random.normal(key_list[15], (2, WIDTH_TWO), jnp.float32), 0.25, 1.75)
    shifts_lower = normal_values(key_list[16], (2, WIDTH_TWO), 0.3, 1.0, jnp.float32)
    return {"noisy_image": noisy_image, "seam_codes": seam_codes, "timestep": timestep, "time_weight": time_weight, "bias_upper": bias_upper, "bias_lower": bias_lower, "kernel_upper_first": kernel_upper_first, "kernel_upper_second": kernel_upper_second, "kernel_lower_first": kernel_lower_first, "kernel_lower_second": kernel_lower_second, "kernel_decode_first": kernel_decode_first, "kernel_decode_second": kernel_decode_second, "output_weight": output_weight, "gains_upper": gains_upper, "shifts_upper": shifts_upper, "gains_lower": gains_lower, "shifts_lower": shifts_lower}


EPSILON = 1e-05

def side_strips(values):
    return jnp.stack([values[:, :, 0, ::-1], values[:, :, ::-1, -1], values[:, :, -1, :], values[:, :, :, 0]], axis=1)

def frame(block_values, upper, lower, west_column, east_column):
    stacked = jnp.concatenate([upper[:, None, :], block_values, lower[:, None, :]], axis=1)
    return jnp.concatenate([west_column[:, :, None], stacked, east_column[:, :, None]], axis=2)

def apply_taps(padded, kernel, height, width):
    channels = padded.shape[0]
    total = jnp.zeros((kernel.shape[2], height * width), jnp.float32)
    for row_off in range(3):
        for col_off in range(3):
            window = padded[:, row_off:row_off + height, col_off:col_off + width].reshape(channels, height * width)
            total = total + jnp.dot(kernel[row_off, col_off], window, preferred_element_type=jnp.float32)
    return total.reshape(kernel.shape[2], height, width)

def convolve(values, seam_codes, kernel):
    tile_count = values.shape[0]
    side_length = values.shape[2]
    edges = side_strips(values)
    offsets = (-ROW_TILES, 1, ROW_TILES, -1)

    def one_tile(place):
        block_values = lax.dynamic_index_in_dim(values, place, 0, False)
        code_row = lax.dynamic_index_in_dim(seam_codes, place, 0, False)
        strip_list = []
        for side_index in range(4):
            neighbour = (place + offsets[side_index]) % tile_count
            facing = (side_index + 2 + code_row[side_index]) % 4
            their_edges = lax.dynamic_index_in_dim(edges, neighbour, 0, False)
            strip_list.append(lax.dynamic_index_in_dim(their_edges, facing, 0, False))
        west_column = jnp.pad(strip_list[3][:, ::-1], ((0, 0), (1, 1)))
        east_column = jnp.pad(strip_list[1], ((0, 0), (1, 1)))
        padded = frame(block_values, strip_list[0], strip_list[2][:, ::-1], west_column, east_column)
        return apply_taps(padded, kernel, side_length, side_length)
    return lax.map(one_tile, jnp.arange(tile_count, dtype=jnp.int32))

def norm_act(values, gain, shift):
    tile_count, channels, height, width = values.shape
    grouped = values.reshape(tile_count, GROUPS, channels // GROUPS, height, width)
    mean = lax.optimization_barrier(jnp.mean(grouped, axis=(0, 2, 3, 4), keepdims=True))
    spread = lax.optimization_barrier(jnp.mean(jnp.square(grouped - mean), axis=(0, 2, 3, 4), keepdims=True))
    normed = ((grouped - mean) / jnp.sqrt(spread + EPSILON)).reshape(values.shape)
    scaled = normed * gain[None, :, None, None] + shift[None, :, None, None]
    return jax.nn.silu(scaled).astype(jnp.bfloat16)

def embedding(timestep, time_weight, bias_upper, bias_lower):
    moment = timestep[0].astype(jnp.float32)
    half_width = time_weight.shape[0] // 2
    frequencies = jnp.exp(-math.log(10000.0) * jnp.arange(half_width, dtype=jnp.float32) / half_width)
    angles = moment * frequencies
    features = jnp.concatenate([jnp.sin(angles), jnp.cos(angles)])[None, :]
    embedded = jax.nn.silu(jnp.dot(features, time_weight, precision=lax.Precision.HIGHEST, preferred_element_type=jnp.float32))
    first_bias = jnp.dot(embedded, bias_upper, precision=lax.Precision.HIGHEST, preferred_element_type=jnp.float32)[0]
    second_bias = jnp.dot(embedded, bias_lower, precision=lax.Precision.HIGHEST, preferred_element_type=jnp.float32)[0]
    return (first_bias, second_bias)

def reference(noisy_image, seam_codes, timestep, time_weight, bias_upper, bias_lower, kernel_upper_first, kernel_upper_second, kernel_lower_first, kernel_lower_second, kernel_decode_first, kernel_decode_second, output_weight, gains_upper, shifts_upper, gains_lower, shifts_lower):
    first_bias, second_bias = embedding(timestep, time_weight, bias_upper, bias_lower)
    first = norm_act(convolve(noisy_image, seam_codes, kernel_upper_first) + first_bias[None, :, None, None], gains_upper[0], shifts_upper[0])
    skip = norm_act(convolve(first, seam_codes, kernel_upper_second), gains_upper[1], shifts_upper[1])
    tile_count, width_one, side_length, _ = skip.shape
    half_side = side_length // 2
    pooled = lax.optimization_barrier(jnp.mean(skip.astype(jnp.float32).reshape(tile_count, width_one, half_side, 2, half_side, 2), axis=(3, 5))).astype(jnp.bfloat16)
    middle = norm_act(convolve(pooled, seam_codes, kernel_lower_first) + second_bias[None, :, None, None], gains_lower[0], shifts_lower[0])
    deep = norm_act(convolve(middle, seam_codes, kernel_lower_second), gains_lower[1], shifts_lower[1])
    widened = jnp.repeat(jnp.repeat(deep, 2, axis=2), 2, axis=3)
    joined = jnp.concatenate([widened, skip], axis=1)
    decoded = norm_act(convolve(joined, seam_codes, kernel_decode_first), gains_upper[2], shifts_upper[2])
    refined = norm_act(convolve(decoded, seam_codes, kernel_decode_second), gains_upper[3], shifts_upper[3])

    def project(place):
        block_values = lax.dynamic_index_in_dim(refined, place, 0, False)
        flat = jnp.dot(output_weight, block_values.reshape(width_one, side_length * side_length), preferred_element_type=jnp.float32)
        return flat.reshape(output_weight.shape[0], side_length, side_length).astype(jnp.bfloat16)
    return lax.map(project, jnp.arange(tile_count, dtype=jnp.int32))
```

```python
import math

import jax
import jax.numpy as jnp
from jax import lax
from jax.experimental import pallas as pl
from jax.experimental.pallas import tpu as pltpu
from jax.sharding import Mesh
from jax.sharding import PartitionSpec as P

GROUPS = 8
ROW_TILES = 4
TILE = ("tile_0", "tile_1", "tile_2", "tile_3")
TILE_SPLIT = ("tile_0", "tile_1", "tile_2", "tile_3", "split")
EPSILON = 1e-05
LANES = 128
F32 = jnp.float32
BF16 = jnp.bfloat16


def lane_index(shape):
    return lax.broadcasted_iota(jnp.int32, shape, 1)


def turn(value, amount):
    return pltpu.roll(value, amount, 1)


def group_index(channels, shape):
    row = lax.broadcasted_iota(jnp.int32, shape, 0)
    return (row * 43) >> (8 if channels == 48 else 9)


def column_of(row_value, channels):
    shape = (channels, row_value.shape[1])
    on_diagonal = lax.broadcasted_iota(jnp.int32, shape, 0) == lane_index(shape)
    return jnp.sum(jnp.where(on_diagonal, jnp.broadcast_to(row_value, shape), 0.0), axis=1, keepdims=True)


def coefficients(stats, gain_row, shift_row, bias_row, channels, pixels):
    devices = stats.shape[0]
    count = pixels * (channels // GROUPS)
    mean_row = jnp.sum(stats, axis=0, keepdims=True) * (1.0 / devices)
    apart = jnp.sum(jnp.square(stats - mean_row), axis=0, keepdims=True) * (1.0 / devices)
    shape = (channels, LANES)
    group = group_index(channels, shape)
    lane = lane_index(shape)

    def pick(row_value, first):
        return jnp.sum(jnp.where(lane == group + first, jnp.broadcast_to(row_value, shape), 0.0), axis=1, keepdims=True)

    mean = pick(mean_row, 0)
    spread = pick(mean_row, GROUPS) * (1.0 / count) + pick(apart, 0)
    slope = lax.rsqrt(spread + EPSILON) * column_of(gain_row, channels)
    offset = column_of(shift_row, channels) - mean * slope
    if bias_row is not None:
        offset = offset + column_of(bias_row, channels) * slope
    return jnp.broadcast_to(slope * 0.5, shape), jnp.broadcast_to(offset * 0.5, shape)


def activate(value, coef):
    half = value.astype(F32) * coef[0] + coef[1]
    return (half + half * jnp.tanh(half)).astype(BF16)


def group_stats(sums, squares, bias_row, channels, pixels, width):
    shape = (channels, LANES)
    lane = lane_index(shape)
    group = group_index(channels, shape)
    inside = lane < width
    mean = jnp.sum(jnp.where(inside, sums, 0.0), axis=1, keepdims=True) * (1.0 / pixels)
    second = jnp.sum(jnp.where(inside, squares, 0.0), axis=1, keepdims=True)
    spread = jnp.maximum(second - pixels * jnp.square(mean), 0.0)
    if bias_row is not None:
        mean = mean + column_of(bias_row, channels)
    group_size = channels // GROUPS
    mean_row = jnp.sum(jnp.where(lane == group, mean, 0.0), axis=0, keepdims=True) * (1.0 / group_size)
    group_mean = jnp.sum(jnp.where(lane == group, mean_row, 0.0), axis=1, keepdims=True)
    total = spread + pixels * jnp.square(mean - group_mean)
    return mean_row + jnp.sum(jnp.where(lane == group + GROUPS, total, 0.0), axis=0, keepdims=True)


def frame_rows(taps, first, channels, width, block_rows, rows_of, upper, lower, west, east, place, together=4):
    stride = taps.shape[1] // 3
    lane = lane_index((channels, LANES))
    base = place * block_rows
    hold_west = turn(west, (LANES + 1 - base) % LANES)
    hold_east = turn(east, (LANES + width - base) % LANES)

    def put(row, value, hw, he):
        taps[row, pl.ds(first, channels)] = jnp.where(lane == 0, hw, turn(value, 1))
        taps[row, pl.ds(stride + first, channels)] = value
        taps[row, pl.ds(2 * stride + first, channels)] = jnp.where(lane == width - 1, he, turn(value, LANES - 1))

    zero = jnp.zeros((channels, LANES), BF16)
    put(0, upper, jnp.where(place == 0, zero, hold_west), jnp.where(place == 0, zero, hold_east))

    def body(step, carry):
        hw, he = carry
        for k in range(together):
            row = step * together + k
            hw, he = turn(hw, LANES - 1), turn(he, LANES - 1)
            put(row + 1, rows_of(row), hw, he)
        return hw, he

    hw, he = lax.fori_loop(0, block_rows // together, body, (hold_west, hold_east))
    hw, he = turn(hw, LANES - 1), turn(he, LANES - 1)
    put(block_rows + 1, lower, jnp.where(place == 1, zero, hw), jnp.where(place == 1, zero, he))


def convolve_rows(taps, weight_ref, raw_ref, block_rows, together=4):
    outputs = weight_ref.shape[0]
    depth = taps.shape[1] * 3
    weight = weight_ref[...]
    zero = jnp.zeros((outputs, LANES), F32)

    def body(step, carry):
        sums, squares = carry
        row = step * together
        for k in range(0, together, 2):
            window = jnp.concatenate(
                [taps[pl.ds(row + k + j, 3)].reshape(depth, LANES) for j in range(2)], axis=1
            )
            both = jnp.dot(weight, window, preferred_element_type=F32)
            for j in range(2):
                value = both[:, j * LANES : (j + 1) * LANES]
                raw_ref[row + k + j] = value
                sums = sums + value
                squares = squares + value * value
        return sums, squares

    return lax.fori_loop(0, block_rows // together, body, (zero, zero))


def pack_edges(raw_ref, pack_ref, block_rows, channels, width, depth, place, together=8):
    size = depth * channels
    lane = lane_index((channels, LANES))
    last = block_rows - 1
    for d in range(depth):
        outer = jnp.where(place == 0, d, last - d)
        pack_ref[pl.ds(d * channels, channels)] = raw_ref[outer].astype(BF16)
        pack_ref[pl.ds(size + d * channels, channels)] = raw_ref[last - outer].astype(BF16)

    def body(step, carry):
        carry = list(carry)
        for k in range(together):
            row = step * together + k
            value = raw_ref[row].astype(F32)
            for d in range(depth):
                line = jnp.where(lane == row, jnp.broadcast_to(value[:, d : d + 1], lane.shape), carry[d])
                right = width - 1 - d
                carry[d] = jnp.where(
                    lane == block_rows + row, jnp.broadcast_to(value[:, right : right + 1], lane.shape), line
                )
        return tuple(carry)

    zero = jnp.zeros((channels, LANES), F32)
    columns = lax.fori_loop(0, block_rows // together, body, (zero,) * depth)
    for d in range(depth):
        pack_ref[pl.ds(2 * size + d * channels, channels)] = columns[d].astype(BF16)


def finish(taps, weight_ref, raw_ref, pack_ref, stat_ref, bias_row, block_rows, channels, width, depth, place):
    sums, squares = convolve_rows(taps, weight_ref, raw_ref, block_rows)
    stat_ref[...] = group_stats(sums, squares, bias_row, channels, float(block_rows * width), width)
    if pack_ref is not None:
        pack_edges(raw_ref, pack_ref, block_rows, channels, width, depth, place)


WHOLE = pl.BlockSpec(memory_space=pltpu.VMEM)
SCALARS = pl.BlockSpec(memory_space=pltpu.SMEM)


def call(body, operands, outs, scratch=()):
    return pl.pallas_call(
        body,
        in_specs=[SCALARS] + [WHOLE] * (len(operands) - 1),
        out_specs=[WHOLE] * len(outs),
        out_shape=[jax.ShapeDtypeStruct(s, d) for s, d in outs],
        scratch_shapes=list(scratch),
        compiler_params=pltpu.CompilerParams(vmem_limit_bytes=48 * 1024 * 1024),
    )(*operands)


def edges_of_image(scalars, image):
    block_rows, channels, width = image.shape

    def body(sc, image_ref, pack_ref):
        pack_edges(image_ref, pack_ref, block_rows, channels, width, 1, sc[0])

    return call(body, (scalars, image), [((3 * channels, LANES), BF16)])[0]


def strips(scalars, pack, partner, width):
    size = pack.shape[0] // 3
    half = width // 2

    def body(sc, mine_ref, their_ref, ns_ref, east_ref, west_ref, side_ref):
        place = sc[0]
        lane = lane_index((size, LANES))

        def ordered(first):
            mine, theirs = mine_ref[pl.ds(first, size)], their_ref[pl.ds(first, size)]
            return jnp.where(place == 0, mine, theirs), jnp.where(place == 0, theirs, mine)

        low, high = ordered(0)
        side_ref[0] = low
        side_ref[2] = high
        low, high = ordered(2 * size)
        side_ref[3] = jnp.where(lane < half, low, turn(high, half))
        side_ref[1] = jnp.where(lane < half, turn(low, LANES - half), high)
        shape = (LANES, LANES)
        row, column = lax.broadcasted_iota(jnp.int32, shape, 0), lane_index(shape)
        for k, out in enumerate((ns_ref, east_ref, west_ref)):
            reverse = sc[2 + 2 * k]
            hit = jnp.where(reverse == 1, width - 1 - row, row) == column
            order = jnp.where(hit & (column < width), 1.0, 0.0).astype(BF16)
            strip = jnp.where(lane < width, side_ref[sc[1 + 2 * k]], jnp.zeros((size, LANES), BF16))
            out[...] = jnp.dot(strip, order, preferred_element_type=F32).astype(BF16)

    outs = [((size, LANES), BF16)] * 3
    return call(body, (scalars, pack, partner), outs, [pltpu.VMEM((4, size, LANES), BF16)])


def above_below(place, facing, inner):
    return jnp.where(place == 0, facing, inner), jnp.where(place == 0, inner, facing)


def first_stage(scalars, image, partner, ns, east, west, weight, bias):
    block_rows, channels, width = image.shape
    outputs = weight.shape[0]

    def body(sc, image_ref, partner_ref, ns_ref, east_ref, west_ref, weight_ref, bias_ref, raw_ref, pack_ref, stat_ref, taps):
        place = sc[0]
        upper, lower = above_below(place, ns_ref[...], partner_ref[pl.ds(channels, channels)])
        frame_rows(
            taps, 0, channels, width, block_rows, lambda r: image_ref[r], upper, lower, west_ref[...], east_ref[...], place
        )
        finish(taps, weight_ref, raw_ref, pack_ref, stat_ref, bias_ref[...], block_rows, outputs, width, 1, place)

    return call(
        body,
        (scalars, image, partner, ns, east, west, weight, bias),
        [((block_rows, outputs, LANES), F32), ((3 * outputs, LANES), BF16), ((1, LANES), F32)],
        [pltpu.VMEM((block_rows + 2, 3 * channels, LANES), BF16)],
    )


def plain_stage(scalars, raw, stats, partner, ns, east, west, weight, gain, shift, bias, width, depth):
    block_rows, channels, _ = raw.shape
    outputs = weight.shape[0]
    biased = bias is not None

    def body(sc, raw_in, stats_ref, partner_ref, ns_ref, east_ref, west_ref, weight_ref, gain_ref, shift_ref, *rest):
        bias_row = None
        if biased:
            bias_row, rest = rest[0][...], rest[1:]
        if depth:
            raw_ref, stat_ref, pack_ref, taps = rest
        else:
            raw_ref, stat_ref, taps = rest
            pack_ref = None
        place = sc[0]
        coef = coefficients(
            stats_ref[...], gain_ref[...], shift_ref[...], bias_row, channels, float(block_rows * width)
        )
        lane = lane_index((channels, LANES))
        clear = jnp.zeros((channels, LANES), BF16)

        def strip(ref):
            return jnp.where(lane < width, activate(ref[...], coef), clear)

        upper, lower = above_below(place, strip(ns_ref), activate(partner_ref[pl.ds(channels, channels)], coef))
        frame_rows(
            taps,
            0,
            channels,
            width,
            block_rows,
            lambda r: activate(raw_in[r], coef),
            upper,
            lower,
            strip(west_ref),
            strip(east_ref),
            place,
        )
        finish(taps, weight_ref, raw_ref, pack_ref, stat_ref, None, block_rows, outputs, width, depth, place)

    outs = [((block_rows, outputs, LANES), F32), ((1, LANES), F32)]
    if depth:
        outs.append(((3 * depth * outputs, LANES), BF16))
    operands = (scalars, raw, stats, partner, ns, east, west, weight, gain, shift)
    if biased:
        operands += (bias,)
    return call(body, operands, outs, [pltpu.VMEM((block_rows + 2, 3 * channels, LANES), BF16)])


def pool_stage(scalars, raw, stats, partner, ns, east, west, weight, gain, shift, bias):
    block_rows, channels, width = raw.shape
    low_rows, low_width = block_rows // 2, width // 2
    outputs = weight.shape[0]

    def body(
        sc, raw_in, stats_ref, partner_ref, ns_ref, east_ref, west_ref, weight_ref, gain_ref, shift_ref, bias_ref,
        skip_ref, side_ref, raw_ref, pack_ref, stat_ref, taps, pooled,
    ):
        place = sc[0]
        coef = coefficients(stats_ref[...], gain_ref[...], shift_ref[...], None, channels, float(block_rows * width))
        shape = (2 * LANES, LANES)
        row, column = lax.broadcasted_iota(jnp.int32, shape, 0), lane_index(shape)
        gather = jnp.where(((row & (LANES - 1)) >> 1) == column, 0.25, 0.0).astype(BF16)

        def pool(outer, second):
            both = jnp.concatenate([outer, second], axis=1)
            return jnp.dot(both, gather, preferred_element_type=F32).astype(BF16)

        def lines(ref, first):
            return activate(ref[pl.ds(first, channels)], coef), activate(ref[pl.ds(first + channels, channels)], coef)

        ns_lines, east_lines, west_lines = lines(ns_ref, 0), lines(east_ref, 0), lines(west_ref, 0)
        inner_lines = lines(partner_ref, 2 * channels)
        upper, lower = above_below(place, ns_lines[0], inner_lines[0])
        side_ref[0] = upper
        side_ref[1] = lower
        side_ref[2] = west_lines[0]
        side_ref[3] = east_lines[0]

        def make(step, carry):
            for k in range(2):
                row = step * 2 + k
                first = activate(raw_in[2 * row], coef)
                second = activate(raw_in[2 * row + 1], coef)
                skip_ref[2 * row] = first
                skip_ref[2 * row + 1] = second
                pooled[row] = pool(first, second)
            return carry

        lax.fori_loop(0, low_rows // 2, make, 0)
        upper, lower = above_below(place, pool(*ns_lines), pool(*inner_lines))
        frame_rows(
            taps,
            0,
            channels,
            low_width,
            low_rows,
            lambda r: pooled[r],
            upper,
            lower,
            pool(*west_lines),
            pool(*east_lines),
            place,
        )
        finish(taps, weight_ref, raw_ref, pack_ref, stat_ref, bias_ref[...], low_rows, outputs, low_width, 1, place)

    return call(
        body,
        (scalars, raw, stats, partner, ns, east, west, weight, gain, shift, bias),
        [
            ((block_rows, channels, LANES), BF16),
            ((4, channels, LANES), BF16),
            ((low_rows, outputs, LANES), F32),
            ((3 * outputs, LANES), BF16),
            ((1, LANES), F32),
        ],
        [pltpu.VMEM((low_rows + 2, 3 * channels, LANES), BF16), pltpu.VMEM((low_rows, channels, LANES), BF16)],
    )


def decode_stage(scalars, raw, stats, partner, ns, east, west, skip, sides, weight, gain, shift):
    low_rows, channels, _ = raw.shape
    block_rows, skip_channels, width = skip.shape
    low_width = width // 2
    joined = channels + skip_channels
    outputs = weight.shape[0]

    def body(
        sc, raw_in, stats_ref, partner_ref, ns_ref, east_ref, west_ref, skip_ref, side_ref, weight_ref, gain_ref, shift_ref,
        raw_ref, pack_ref, stat_ref, taps, wide,
    ):
        place = sc[0]
        coef = coefficients(
            stats_ref[...], gain_ref[...], shift_ref[...], None, channels, float(low_rows * low_width)
        )
        shape = (LANES, LANES)
        row, column = lax.broadcasted_iota(jnp.int32, shape, 0), lane_index(shape)
        spread = jnp.where(row == column >> 1, 1.0, 0.0).astype(BF16)

        lane = lane_index((channels, LANES))

        def widen(value):
            kept = jnp.where(lane < low_width, activate(value, coef), jnp.zeros((channels, LANES), BF16))
            return jnp.dot(kept, spread, preferred_element_type=F32).astype(BF16)

        def make(step, carry):
            for k in range(4):
                row = step * 4 + k
                wide[row] = widen(raw_in[row])
            return carry

        lax.fori_loop(0, low_rows // 4, make, 0)
        upper, lower = above_below(place, widen(ns_ref[...]), widen(partner_ref[pl.ds(channels, channels)]))
        frame_rows(
            taps,
            0,
            channels,
            width,
            block_rows,
            lambda r: wide[r >> 1],
            upper,
            lower,
            widen(west_ref[...]),
            widen(east_ref[...]),
            place,
            2,
        )
        frame_rows(
            taps,
            channels,
            skip_channels,
            width,
            block_rows,
            lambda r: skip_ref[r],
            side_ref[0],
            side_ref[1],
            side_ref[2],
            side_ref[3],
            place,
        )
        finish(taps, weight_ref, raw_ref, pack_ref, stat_ref, None, block_rows, outputs, width, 1, place)

    return call(
        body,
        (scalars, raw, stats, partner, ns, east, west, skip, sides, weight, gain, shift),
        [((block_rows, outputs, LANES), F32), ((3 * outputs, LANES), BF16), ((1, LANES), F32)],
        [pltpu.VMEM((block_rows + 2, 3 * joined, LANES), BF16), pltpu.VMEM((low_rows, channels, LANES), BF16)],
    )


def project_stage(scalars, raw, stats, weight, gain, shift, kept):
    block_rows, channels, width = raw.shape

    def body(sc, raw_in, stats_ref, weight_ref, gain_ref, shift_ref, out_ref):
        coef = coefficients(stats_ref[...], gain_ref[...], shift_ref[...], None, channels, float(block_rows * width))
        project = weight_ref[...]

        def make(step, carry):
            for k in range(0, 4, 2):
                row = step * 4 + k
                both = jnp.concatenate([activate(raw_in[row], coef), activate(raw_in[row + 1], coef)], axis=1)
                result = jnp.dot(project, both, preferred_element_type=F32).astype(BF16)
                out_ref[row] = result[:kept, :LANES]
                out_ref[row + 1] = result[:kept, LANES:]
            return carry

        lax.fori_loop(0, block_rows // 4, make, 0)

    return call(body, (scalars, raw, stats, weight, gain, shift), [((block_rows, kept, LANES), BF16)])[0]


def shift_tiles(value, steps):
    count = lax.axis_size(TILE)
    return lax.ppermute(value, TILE, [(t, (t + steps) % count) for t in range(count)])


def vertical(value):
    count = lax.axis_size(TILE)
    pairs = []
    for t in range(count):
        pairs.append((2 * t, 2 * ((t + ROW_TILES) % count)))
        pairs.append((2 * t + 1, 2 * ((t - ROW_TILES) % count) + 1))
    return lax.ppermute(value, TILE_SPLIT, pairs)


def exchange(scalars, pack, width):
    partner = lax.ppermute(pack, "split", [(0, 1), (1, 0)])
    ns, east, west = strips(scalars, pack, partner, width)
    return partner, vertical(ns), shift_tiles(east, -1), shift_tiles(west, 1)


def share(stat):
    devices = lax.axis_size(TILE) * lax.axis_size("split")
    copies = jnp.broadcast_to(stat[None], (devices, 1, LANES))
    return lax.all_to_all(copies, TILE_SPLIT, 0, 0).reshape(devices, LANES)


def embedding(timestep, time_weight, bias_upper, bias_lower):
    moment = timestep[0].astype(F32)
    half_width = time_weight.shape[0] // 2
    frequencies = jnp.exp(-math.log(10000.0) * jnp.arange(half_width, dtype=F32) / half_width)
    angles = moment * frequencies
    features = jnp.concatenate([jnp.sin(angles), jnp.cos(angles)])[None, :]
    embedded = jax.nn.silu(jnp.dot(features, time_weight, precision=lax.Precision.HIGHEST))
    both = jnp.concatenate([bias_upper, bias_lower], axis=1)
    biases = jnp.dot(embedded, both, precision=lax.Precision.HIGHEST)
    return biases[:, : bias_upper.shape[1]], biases[:, bias_upper.shape[1] :]


def flat_kernel(kernel):
    return jnp.transpose(kernel, (2, 0, 1, 3)).reshape(kernel.shape[2], -1)


def seam_scalars(seam_codes):
    count = lax.axis_size(TILE)
    tile, place = lax.axis_index(TILE), lax.axis_index("split")

    def facing(target, side):
        k = (side + 2 + seam_codes[target % count, side]) % 4
        reverse = (k < 2) == (side < 2)
        return k, reverse.astype(jnp.int32)

    north = facing(tile + ROW_TILES, 0)
    south = facing(tile - ROW_TILES, 2)
    up = place == 0
    vertical_pick = (jnp.where(up, north[0], south[0]), jnp.where(up, north[1], south[1]))
    picks = vertical_pick + facing(tile - 1, 1) + facing(tile + 1, 3)
    return jnp.stack([place] + [p.astype(jnp.int32) for p in picks])


def per_device(
    noisy_image,
    seam_codes,
    timestep,
    time_weight,
    bias_upper,
    bias_lower,
    kernel_upper_first,
    kernel_upper_second,
    kernel_lower_first,
    kernel_lower_second,
    kernel_decode_first,
    kernel_decode_second,
    output_weight,
    gains_upper,
    shifts_upper,
    gains_lower,
    shifts_lower,
):
    scalars = seam_scalars(seam_codes)
    first_bias, second_bias = embedding(timestep, time_weight, bias_upper, bias_lower)
    channels, block_rows, width = noisy_image.shape[1:]
    padding = kernel_upper_first.shape[2] - channels
    image = jnp.transpose(jnp.pad(noisy_image[0], ((0, padding), (0, 0), (0, 0))), (1, 0, 2))
    upper_first = flat_kernel(jnp.pad(kernel_upper_first, ((0, 0), (0, 0), (0, 0), (0, padding))))
    low_width = width // 2

    pack = edges_of_image(scalars, image)
    received = exchange(scalars, pack, width)
    raw, pack, stat = first_stage(scalars, image, *received, upper_first, first_bias)

    stats, received = share(stat), exchange(scalars, pack, width)
    raw, stat, pack = plain_stage(
        scalars, raw, stats, *received, flat_kernel(kernel_upper_second), gains_upper[0:1], shifts_upper[0:1], first_bias,
        width, 2,
    )

    stats, received = share(stat), exchange(scalars, pack, width)
    skip, sides, raw, pack, stat = pool_stage(
        scalars, raw, stats, *received, flat_kernel(kernel_lower_first), gains_upper[1:2], shifts_upper[1:2], second_bias
    )

    stats, received = share(stat), exchange(scalars, pack, low_width)
    raw, stat, pack = plain_stage(
        scalars, raw, stats, *received, flat_kernel(kernel_lower_second), gains_lower[0:1], shifts_lower[0:1], second_bias,
        low_width, 1,
    )

    stats, received = share(stat), exchange(scalars, pack, low_width)
    raw, pack, stat = decode_stage(
        scalars, raw, stats, *received, skip, sides, flat_kernel(kernel_decode_first), gains_lower[1:2], shifts_lower[1:2]
    )

    stats, received = share(stat), exchange(scalars, pack, width)
    raw, stat = plain_stage(
        scalars, raw, stats, *received, flat_kernel(kernel_decode_second), gains_upper[2:3], shifts_upper[2:3], None, width, 0
    )

    project = jnp.pad(output_weight, ((0, padding), (0, 0)))
    result = project_stage(scalars, raw, share(stat), project, gains_upper[3:4], shifts_upper[3:4], channels)
    return jnp.transpose(result, (1, 0, 2))[None]


def solution(mesh):
    torus = Mesh(
        mesh.devices.reshape(4, 4, 2, 2, mesh.shape["split"]),
        ("tile_0", "tile_1", "tile_2", "tile_3", "split"),
    )
    return jax.shard_map(
        per_device,
        mesh=torus,
        in_specs=(P(TILE, None, "split", None),) + (P(),) * 16,
        out_specs=P(TILE, None, "split", None),
        check_vma=False,
    )
```

```python
import math

import jax
import jax.numpy as jnp
from jax import lax
from jax.experimental import pallas as pl
from jax.experimental.pallas import tpu as pltpu
from jax.sharding import Mesh
from jax.sharding import PartitionSpec as P


GROUPS = 8
ROW_TILES = 4
TILE = ("tile_0", "tile_1", "tile_2", "tile_3")
TILE_SPLIT = ("tile_0", "tile_1", "tile_2", "tile_3", "split")
EPSILON = 1e-05
LANES = 128
DEVICES = 128
F32 = jnp.float32
BF16 = jnp.bfloat16


def lane_index(shape):
    return lax.broadcasted_iota(jnp.int32, shape, 1)


def turn(value, amount):
    return pltpu.roll(value, amount, 1)


def group_index(channels, shape):
    row = lax.broadcasted_iota(jnp.int32, shape, 0)
    return (row * 43) >> (8 if channels == 48 else 9)


def column_of(row_value, channels, first=0):
    shape = (channels, row_value.shape[1])
    on_diagonal = lax.broadcasted_iota(jnp.int32, shape, 0) + first == lane_index(shape)
    return jnp.sum(jnp.where(on_diagonal, jnp.broadcast_to(row_value, shape), 0.0), axis=1, keepdims=True)


def coefficients(stats, gain_row, shift_row, bias, channels, pixels):
    devices = stats.shape[0]
    count = pixels * (channels // GROUPS)
    mean_row = jnp.sum(stats, axis=0, keepdims=True) * (1.0 / devices)
    apart = jnp.sum(jnp.square(stats - mean_row), axis=0, keepdims=True) * (1.0 / devices)
    shape = (channels, LANES)
    group = group_index(channels, shape)
    lane = lane_index(shape)

    def pick(row_value, first):
        return jnp.sum(jnp.where(lane == group + first, jnp.broadcast_to(row_value, shape), 0.0), axis=1, keepdims=True)

    mean = pick(mean_row, 0)
    spread = pick(mean_row, GROUPS) * (1.0 / count) + pick(apart, 0)
    slope = lax.rsqrt(spread + EPSILON) * column_of(gain_row, channels)
    offset = column_of(shift_row, channels) - mean * slope
    if bias is not None:
        offset = offset + column_of(bias[0][...], channels, bias[1]) * slope
    return jnp.broadcast_to(slope * 0.5, shape), jnp.broadcast_to(offset * 0.5, shape)


def activate(value, coef):
    half = value.astype(F32) * coef[0] + coef[1]
    return (half + half * jnp.tanh(half)).astype(BF16)


def group_stats(sums, squares, bias, channels, pixels, width):
    shape = (channels, LANES)
    lane = lane_index(shape)
    group = group_index(channels, shape)
    inside = lane < width
    mean = jnp.sum(jnp.where(inside, sums, 0.0), axis=1, keepdims=True) * (1.0 / pixels)
    second = jnp.sum(jnp.where(inside, squares, 0.0), axis=1, keepdims=True)
    spread = jnp.maximum(second - pixels * jnp.square(mean), 0.0)
    if bias is not None:
        mean = mean + column_of(bias[0][...], channels, bias[1])
    group_size = channels // GROUPS
    mean_row = jnp.sum(jnp.where(lane == group, mean, 0.0), axis=0, keepdims=True) * (1.0 / group_size)
    group_mean = jnp.sum(jnp.where(lane == group, mean_row, 0.0), axis=1, keepdims=True)
    total = spread + pixels * jnp.square(mean - group_mean)
    return mean_row + jnp.sum(jnp.where(lane == group + GROUPS, total, 0.0), axis=0, keepdims=True)


def frame_rows(taps, first, channels, width, block_rows, rows_of, upper, lower, west, east, place, together=4):
    stride = taps.shape[1] // 3
    lane = lane_index((channels, LANES))
    base = place * block_rows

    def put(row, value, hw, he):
        taps[row, pl.ds(first, channels)] = jnp.where(lane == 0, hw, turn(value, 1))
        taps[row, pl.ds(stride + first, channels)] = value
        taps[row, pl.ds(2 * stride + first, channels)] = jnp.where(lane == width - 1, he, turn(value, LANES - 1))

    def sides(row):
        return turn(west, (LANES - base - row) % LANES), turn(east, (2 * LANES + width - 1 - base - row) % LANES)

    zero = jnp.zeros((channels, LANES), BF16)
    hw, he = sides(-1)
    put(0, upper, jnp.where(place == 0, zero, hw), jnp.where(place == 0, zero, he))

    def body(step, carry):
        for k in range(together):
            row = step * together + k
            put(row + 1, rows_of(row), *sides(row))
        return carry

    lax.fori_loop(0, block_rows // together, body, 0)
    hw, he = sides(block_rows)
    put(block_rows + 1, lower, jnp.where(place == 1, zero, hw), jnp.where(place == 1, zero, he))


def convolve_rows(taps, weight_ref, raw_ref, block_rows, together=4):
    outputs = weight_ref.shape[0]
    depth = taps.shape[1] * 3
    weight = weight_ref[...]
    zero = jnp.zeros((outputs, LANES), F32)

    def body(step, carry):
        sums, squares = carry
        row = step * together
        for k in range(0, together, 2):
            window = jnp.concatenate(
                [taps[pl.ds(row + k + j, 3)].reshape(depth, LANES) for j in range(2)], axis=1
            )
            both = jnp.dot(weight, window, preferred_element_type=F32)
            for j in range(2):
                value = both[:, j * LANES : (j + 1) * LANES]
                raw_ref[row + k + j] = value.astype(BF16)
                sums = sums + value
                squares = squares + value * value
        return sums, squares

    return lax.fori_loop(0, block_rows // together, body, (zero, zero))


def pack_edges(raw_ref, pack_ref, block_rows, channels, width, depth, place, together=8):
    size = depth * channels
    lane = lane_index((channels, LANES))
    last = block_rows - 1
    for d in range(depth):
        outer = jnp.where(place == 0, d, last - d)
        pack_ref[pl.ds(d * channels, channels)] = raw_ref[outer].astype(BF16)
        pack_ref[pl.ds(size + d * channels, channels)] = raw_ref[last - outer].astype(BF16)

    spacing = 2 if width == LANES else 1

    def body(step, carry):
        carry = list(carry)
        for k in range(together):
            row = step * together + k
            value = raw_ref[row].astype(BF16)
            for d in range(depth):
                amount = spacing * row
                west = (lane == amount)
                east = lane == (amount + width - 1) % LANES
                if d:
                    left = turn(value, (amount + LANES - d) % LANES)
                    right = turn(value, (amount + d) % LANES)
                    carry[d] = jnp.where(west, left, jnp.where(east, right, carry[d]))
                else:
                    carry[d] = jnp.where(west | east, turn(value, amount), carry[d])
        return tuple(carry)

    zero = jnp.zeros((channels, LANES), BF16)
    columns = lax.fori_loop(0, block_rows // together, body, (zero,) * depth)
    for d in range(depth):
        pack_ref[pl.ds(2 * size + d * channels, channels)] = columns[d]


def finish(taps, weight_ref, raw_ref, pack_ref, stat_ref, bias, block_rows, channels, width, depth, place):
    sums, squares = convolve_rows(taps, weight_ref, raw_ref, block_rows)
    stat = group_stats(sums, squares, bias, channels, float(block_rows * width), width)
    stat_ref[...] = jnp.broadcast_to(stat, stat_ref.shape)
    if pack_ref is not None:
        pack_edges(raw_ref, pack_ref, block_rows, channels, width, depth, place)


WHOLE = pl.BlockSpec(memory_space=pltpu.VMEM)
SCALARS = pl.BlockSpec(memory_space=pltpu.SMEM)


def call(body, operands, outs, scratch=(), limit=12):
    return pl.pallas_call(
        body,
        in_specs=[SCALARS] + [WHOLE] * (len(operands) - 1),
        out_specs=[WHOLE] * len(outs),
        out_shape=[jax.ShapeDtypeStruct(s, d) for s, d in outs],
        scratch_shapes=list(scratch),
        compiler_params=pltpu.CompilerParams(vmem_limit_bytes=limit * 1024 * 1024),
    )(*operands)


def edges_of_image(scalars, image):
    block_rows, channels, width = image.shape

    def body(sc, image_ref, pack_ref):
        pack_edges(image_ref, pack_ref, block_rows, channels, width, 1, sc[0])

    return call(body, (scalars, image), [((3 * channels, LANES), BF16)])[0]


def strips(scalars, pack, partner, width):
    size = pack.shape[0] // 3
    half = width // 2

    def body(sc, mine_ref, their_ref, ns_ref, east_ref, west_ref, side_ref):
        place = sc[0]
        lane = lane_index((size, LANES))

        def ordered(first):
            mine, theirs = mine_ref[pl.ds(first, size)], their_ref[pl.ds(first, size)]
            return jnp.where(place == 0, mine, theirs), jnp.where(place == 0, theirs, mine)

        low, high = ordered(0)
        side_ref[0] = low
        side_ref[2] = high
        shape = (LANES, LANES)
        row, column = lax.broadcasted_iota(jnp.int32, shape, 0), lane_index(shape)
        low, high = ordered(2 * size)
        both = jnp.concatenate([low, high], axis=1)
        spacing = 2 if width == LANES else 1
        for side, start in ((3, 0), (1, width - 1)):
            upper = (row == (start + spacing * column) % LANES) & (column < half)
            under = (row == (start + spacing * (column - half)) % LANES) & (column >= half) & (column < width)
            spread = jnp.concatenate([upper, under], axis=0)
            spread = jnp.where(spread, 1.0, 0.0).astype(BF16)
            side_ref[side] = jnp.dot(both, spread, preferred_element_type=F32).astype(BF16)
        for k, out in enumerate((ns_ref, east_ref, west_ref)):
            reverse = sc[2 + 2 * k]
            hit = jnp.where(reverse == 1, width - 1 - row, row) == column
            order = jnp.where(hit & (column < width), 1.0, 0.0).astype(BF16)
            strip = jnp.where(lane < width, side_ref[sc[1 + 2 * k]], jnp.zeros((size, LANES), BF16))
            out[...] = jnp.dot(strip, order, preferred_element_type=F32).astype(BF16)

    outs = [((size, LANES), BF16)] * 3
    return call(body, (scalars, pack, partner), outs, [pltpu.VMEM((4, size, LANES), BF16)])


def above_below(place, facing, inner):
    return jnp.where(place == 0, facing, inner), jnp.where(place == 0, inner, facing)


def first_stage(scalars, image, partner, ns, east, west, weight, bias):
    block_rows, channels, width = image.shape
    outputs = weight.shape[0]

    def body(sc, image_ref, partner_ref, ns_ref, east_ref, west_ref, weight_ref, bias_ref, raw_ref, pack_ref, stat_ref, taps):
        place = sc[0]
        upper, lower = above_below(place, ns_ref[...], partner_ref[pl.ds(channels, channels)])
        frame_rows(
            taps, 0, channels, width, block_rows, lambda r: image_ref[r], upper, lower, west_ref[...], east_ref[...], place
        )
        finish(taps, weight_ref, raw_ref, pack_ref, stat_ref, (bias_ref, 0), block_rows, outputs, width, 1, place)

    return call(
        body,
        (scalars, image, partner, ns, east, west, weight, bias),
        [((block_rows, outputs, LANES), BF16), ((3 * outputs, LANES), BF16), ((DEVICES, LANES), F32)],
        [pltpu.VMEM((block_rows + 2, 3 * channels, LANES), BF16)],
    )


def plain_stage(scalars, raw, stats, partner, ns, east, west, weight, gain, shift, line, bias, first, width, depth):
    block_rows, channels, _ = raw.shape
    outputs = weight.shape[0]
    biased = bias is not None

    def body(sc, raw_in, stats_ref, partner_ref, ns_ref, east_ref, west_ref, weight_ref, gain_ref, shift_ref, *rest):
        bias_row = None
        if biased:
            bias_row, rest = (rest[0], first), rest[1:]
        if depth:
            raw_ref, stat_ref, pack_ref, taps = rest
        else:
            raw_ref, stat_ref, taps = rest
            pack_ref = None
        place = sc[0]
        coef = coefficients(
            stats_ref[...], gain_ref[line : line + 1], shift_ref[line : line + 1], bias_row, channels, float(block_rows * width)
        )
        lane = lane_index((channels, LANES))
        clear = jnp.zeros((channels, LANES), BF16)

        def strip(ref):
            return jnp.where(lane < width, activate(ref[...], coef), clear)

        upper, lower = above_below(place, strip(ns_ref), activate(partner_ref[pl.ds(channels, channels)], coef))
        frame_rows(
            taps,
            0,
            channels,
            width,
            block_rows,
            lambda r: activate(raw_in[r], coef),
            upper,
            lower,
            strip(west_ref),
            strip(east_ref),
            place,
        )
        finish(taps, weight_ref, raw_ref, pack_ref, stat_ref, None, block_rows, outputs, width, depth, place)

    outs = [((block_rows, outputs, LANES), BF16), ((DEVICES, LANES), F32)]
    if depth:
        outs.append(((3 * depth * outputs, LANES), BF16))
    operands = (scalars, raw, stats, partner, ns, east, west, weight, gain, shift)
    if biased:
        operands += (bias,)
    return call(body, operands, outs, [pltpu.VMEM((block_rows + 2, 3 * channels, LANES), BF16)])


def pool_stage(scalars, raw, stats, partner, ns, east, west, weight, gain, shift, bias):
    block_rows, channels, width = raw.shape
    low_rows, low_width = block_rows // 2, width // 2
    outputs = weight.shape[0]

    def body(
        sc, raw_in, stats_ref, partner_ref, ns_ref, east_ref, west_ref, weight_ref, gain_ref, shift_ref, bias_ref,
        skip_ref, side_ref, raw_ref, pack_ref, stat_ref, taps, pooled,
    ):
        place = sc[0]
        coef = coefficients(stats_ref[...], gain_ref[1:2], shift_ref[1:2], None, channels, float(block_rows * width))
        shape = (2 * LANES, LANES)
        row, column = lax.broadcasted_iota(jnp.int32, shape, 0), lane_index(shape)
        gather = jnp.where(((row & (LANES - 1)) >> 1) == column, 0.25, 0.0).astype(BF16)

        def pool(outer, second):
            both = jnp.concatenate([outer, second], axis=1)
            return jnp.dot(both, gather, preferred_element_type=F32).astype(BF16)

        def lines(ref, first):
            return activate(ref[pl.ds(first, channels)], coef), activate(ref[pl.ds(first + channels, channels)], coef)

        ns_lines, east_lines, west_lines = lines(ns_ref, 0), lines(east_ref, 0), lines(west_ref, 0)
        inner_lines = lines(partner_ref, 2 * channels)
        upper, lower = above_below(place, ns_lines[0], inner_lines[0])
        side_ref[0] = upper
        side_ref[1] = lower
        side_ref[2] = west_lines[0]
        side_ref[3] = east_lines[0]

        def make(step, carry):
            for k in range(2):
                row = step * 2 + k
                first = activate(raw_in[2 * row], coef)
                second = activate(raw_in[2 * row + 1], coef)
                skip_ref[2 * row] = first
                skip_ref[2 * row + 1] = second
                pooled[row] = pool(first, second)
            return carry

        lax.fori_loop(0, low_rows // 2, make, 0)
        upper, lower = above_below(place, pool(*ns_lines), pool(*inner_lines))
        frame_rows(
            taps,
            0,
            channels,
            low_width,
            low_rows,
            lambda r: pooled[r],
            upper,
            lower,
            pool(*west_lines),
            pool(*east_lines),
            place,
        )
        finish(taps, weight_ref, raw_ref, pack_ref, stat_ref, (bias_ref, channels), low_rows, outputs, low_width, 1, place)

    return call(
        body,
        (scalars, raw, stats, partner, ns, east, west, weight, gain, shift, bias),
        [
            ((block_rows, channels, LANES), BF16),
            ((4, channels, LANES), BF16),
            ((low_rows, outputs, LANES), BF16),
            ((3 * outputs, LANES), BF16),
            ((DEVICES, LANES), F32),
        ],
        [pltpu.VMEM((low_rows + 2, 3 * channels, LANES), BF16), pltpu.VMEM((low_rows, channels, LANES), BF16)],
    )


def decode_stage(scalars, raw, stats, partner, ns, east, west, skip, sides, weight, gain, shift):
    low_rows, channels, _ = raw.shape
    block_rows, skip_channels, width = skip.shape
    low_width = width // 2
    joined = channels + skip_channels
    outputs = weight.shape[0]

    def body(
        sc, raw_in, stats_ref, partner_ref, ns_ref, east_ref, west_ref, skip_ref, side_ref, weight_ref, gain_ref, shift_ref,
        raw_ref, pack_ref, stat_ref, taps, wide,
    ):
        place = sc[0]
        coef = coefficients(
            stats_ref[...], gain_ref[1:2], shift_ref[1:2], None, channels, float(low_rows * low_width)
        )
        shape = (LANES, LANES)
        row, column = lax.broadcasted_iota(jnp.int32, shape, 0), lane_index(shape)
        spread = jnp.where(row == column >> 1, 1.0, 0.0).astype(BF16)

        lane = lane_index((channels, LANES))

        def widen(value):
            kept = jnp.where(lane < low_width, activate(value, coef), jnp.zeros((channels, LANES), BF16))
            return jnp.dot(kept, spread, preferred_element_type=F32).astype(BF16)

        def make(step, carry):
            for k in range(4):
                row = step * 4 + k
                wide[row] = widen(raw_in[row])
            return carry

        lax.fori_loop(0, low_rows // 4, make, 0)
        upper, lower = above_below(place, widen(ns_ref[...]), widen(partner_ref[pl.ds(channels, channels)]))
        frame_rows(
            taps,
            0,
            channels,
            width,
            block_rows,
            lambda r: wide[r >> 1],
            upper,
            lower,
            widen(west_ref[...]),
            widen(east_ref[...]),
            place,
            2,
        )
        frame_rows(
            taps,
            channels,
            skip_channels,
            width,
            block_rows,
            lambda r: skip_ref[r],
            side_ref[0],
            side_ref[1],
            side_ref[2],
            side_ref[3],
            place,
        )
        finish(taps, weight_ref, raw_ref, pack_ref, stat_ref, None, block_rows, outputs, width, 1, place)

    return call(
        body,
        (scalars, raw, stats, partner, ns, east, west, skip, sides, weight, gain, shift),
        [((block_rows, outputs, LANES), BF16), ((3 * outputs, LANES), BF16), ((DEVICES, LANES), F32)],
        [pltpu.VMEM((block_rows + 2, 3 * joined, LANES), BF16), pltpu.VMEM((low_rows, channels, LANES), BF16)],
        20,
    )


def project_stage(scalars, raw, stats, weight, gain, shift, kept):
    block_rows, channels, width = raw.shape

    def body(sc, raw_in, stats_ref, weight_ref, gain_ref, shift_ref, out_ref):
        coef = coefficients(stats_ref[...], gain_ref[3:4], shift_ref[3:4], None, channels, float(block_rows * width))
        project = weight_ref[...]

        def make(step, carry):
            for k in range(0, 4, 2):
                row = step * 4 + k
                both = jnp.concatenate([activate(raw_in[row], coef), activate(raw_in[row + 1], coef)], axis=1)
                result = jnp.dot(project, both, preferred_element_type=F32).astype(BF16)
                out_ref[row] = result[:kept, :LANES]
                out_ref[row + 1] = result[:kept, LANES:]
            return carry

        lax.fori_loop(0, block_rows // 4, make, 0)

    return call(body, (scalars, raw, stats, weight, gain, shift), [((block_rows, kept, LANES), BF16)])[0]


def shift_tiles(value, steps):
    count = lax.axis_size(TILE)
    return lax.ppermute(value, TILE, [(t, (t + steps) % count) for t in range(count)])


def vertical(value):
    count = lax.axis_size(TILE)
    pairs = []
    for t in range(count):
        pairs.append((2 * t, 2 * ((t + ROW_TILES) % count)))
        pairs.append((2 * t + 1, 2 * ((t - ROW_TILES) % count) + 1))
    return lax.ppermute(value, TILE_SPLIT, pairs)


def exchange(scalars, pack, width):
    partner = lax.ppermute(pack, "split", [(0, 1), (1, 0)])
    ns, east, west = strips(scalars, pack, partner, width)
    west = shift_tiles(west, 1)
    east = shift_tiles(east, -1)
    ns = vertical(ns)
    return partner, ns, east, west


def share(stat):
    copies = stat.reshape(DEVICES, 1, LANES)
    return lax.all_to_all(copies, TILE_SPLIT, 0, 0).reshape(DEVICES, LANES)


def meet(scalars, pack, stat, width):
    received = exchange(scalars, pack, width) if pack is not None else None
    return (share(stat) if stat is not None else None), received


def embedding(timestep, time_weight, bias_upper, bias_lower):
    moment = timestep[0].astype(F32)
    half_width = time_weight.shape[0] // 2
    frequencies = jnp.exp(-math.log(10000.0) * jnp.arange(half_width, dtype=F32) / half_width)
    angles = moment * frequencies
    features = jnp.concatenate([jnp.sin(angles), jnp.cos(angles)])[None, :]
    embedded = jax.nn.silu(jnp.dot(features, time_weight, precision=lax.Precision.HIGHEST))
    both = jnp.concatenate([bias_upper, bias_lower], axis=1)
    biases = jnp.dot(embedded, both, precision=lax.Precision.HIGHEST)
    return biases


def flat_kernel(kernel):
    return jnp.transpose(kernel, (2, 0, 1, 3)).reshape(kernel.shape[2], -1)


def seam_scalars(seam_codes):
    count = lax.axis_size(TILE)
    tile, place = lax.axis_index(TILE), lax.axis_index("split")

    def facing(target, side):
        k = (side + 2 + seam_codes[target % count, side]) % 4
        reverse = (k < 2) == (side < 2)
        return k, reverse.astype(jnp.int32)

    north = facing(tile + ROW_TILES, 0)
    south = facing(tile - ROW_TILES, 2)
    up = place == 0
    vertical_pick = (jnp.where(up, north[0], south[0]), jnp.where(up, north[1], south[1]))
    picks = vertical_pick + facing(tile - 1, 1) + facing(tile + 1, 3)
    return jnp.stack([place] + [p.astype(jnp.int32) for p in picks])


def per_device(
    noisy_image,
    seam_codes,
    timestep,
    time_weight,
    bias_upper,
    bias_lower,
    kernel_upper_first,
    kernel_upper_second,
    kernel_lower_first,
    kernel_lower_second,
    kernel_decode_first,
    kernel_decode_second,
    output_weight,
    gains_upper,
    shifts_upper,
    gains_lower,
    shifts_lower,
):
    scalars = seam_scalars(seam_codes)
    biases = embedding(timestep, time_weight, bias_upper, bias_lower)
    channels, _, width = noisy_image.shape[1:]
    padding = kernel_upper_first.shape[2] - channels
    image = jnp.transpose(jnp.pad(noisy_image[0], ((0, padding), (0, 0), (0, 0))), (1, 0, 2))
    upper_first = flat_kernel(jnp.pad(kernel_upper_first, ((0, 0), (0, 0), (0, 0), (0, padding))))
    low_width = width // 2
    width_one = kernel_upper_first.shape[2]

    pack = edges_of_image(scalars, image)
    _, received = meet(scalars, pack, None, width)
    raw, pack, stat = first_stage(scalars, image, *received, upper_first, biases)

    stats, received = meet(scalars, pack, stat, width)
    raw, stat, pack = plain_stage(
        scalars, raw, stats, *received, flat_kernel(kernel_upper_second), gains_upper, shifts_upper, 0, biases, 0, width, 2
    )

    stats, received = meet(scalars, pack, stat, width)
    skip, sides, raw, pack, stat = pool_stage(
        scalars, raw, stats, *received, flat_kernel(kernel_lower_first), gains_upper, shifts_upper, biases
    )

    stats, received = meet(scalars, pack, stat, low_width)
    raw, stat, pack = plain_stage(
        scalars, raw, stats, *received, flat_kernel(kernel_lower_second), gains_lower, shifts_lower, 0, biases, width_one,
        low_width, 1,
    )

    stats, received = meet(scalars, pack, stat, low_width)
    raw, pack, stat = decode_stage(
        scalars, raw, stats, *received, skip, sides, flat_kernel(kernel_decode_first), gains_lower, shifts_lower
    )

    stats, received = meet(scalars, pack, stat, width)
    raw, stat = plain_stage(
        scalars, raw, stats, *received, flat_kernel(kernel_decode_second), gains_upper, shifts_upper, 2, None, 0, width, 0
    )

    stats, _ = meet(scalars, None, stat, width)
    project = jnp.pad(output_weight, ((0, padding), (0, 0)))
    result = project_stage(scalars, raw, stats, project, gains_upper, shifts_upper, channels)
    return jnp.transpose(result, (1, 0, 2))[None]


def solution(mesh):
    torus = Mesh(
        mesh.devices.reshape(4, 4, 2, 2, mesh.shape["split"]),
        ("tile_0", "tile_1", "tile_2", "tile_3", "split"),
    )
    return jax.shard_map(
        per_device,
        mesh=torus,
        in_specs=(P(TILE, None, "split", None),) + (P(),) * 16,
        out_specs=P(TILE, None, "split", None),
        check_vma=False,
    )
```

```python
import math

import jax
import jax.numpy as jnp
from jax import lax
from jax.experimental import pallas as pl
from jax.experimental.pallas import tpu as pltpu
from jax.sharding import Mesh
from jax.sharding import PartitionSpec as P


GROUPS = 8
ROW_TILES = 4
TILE = ("tile_0", "tile_1", "tile_2", "tile_3")
TILE_SPLIT = ("tile_0", "tile_1", "tile_2", "tile_3", "split")
EPSILON = 1e-05
LANES = 128
DEVICES = 128
F32 = jnp.float32
BF16 = jnp.bfloat16


def lane_index(shape):
    return lax.broadcasted_iota(jnp.int32, shape, 1)


def turn(value, amount):
    return pltpu.roll(value, amount, 1)


def group_index(channels, shape):
    row = lax.broadcasted_iota(jnp.int32, shape, 0)
    return (row * 43) >> (8 if channels == 48 else 9)


def column_of(row_value, channels, first=0):
    shape = (channels, row_value.shape[1])
    on_diagonal = lax.broadcasted_iota(jnp.int32, shape, 0) + first == lane_index(shape)
    return jnp.sum(jnp.where(on_diagonal, jnp.broadcast_to(row_value, shape), 0.0), axis=1, keepdims=True)


def coefficients(stats, gain_row, shift_row, bias, channels, pixels):
    devices = stats.shape[0]
    count = pixels * (channels // GROUPS)
    mean_row = jnp.sum(stats, axis=0, keepdims=True) * (1.0 / devices)
    apart = jnp.sum(jnp.square(stats - mean_row), axis=0, keepdims=True) * (1.0 / devices)
    shape = (channels, LANES)
    group = group_index(channels, shape)
    lane = lane_index(shape)

    def pick(row_value, first):
        return jnp.sum(jnp.where(lane == group + first, jnp.broadcast_to(row_value, shape), 0.0), axis=1, keepdims=True)

    mean = pick(mean_row, 0)
    spread = pick(mean_row, GROUPS) * (1.0 / count) + pick(apart, 0)
    slope = lax.rsqrt(spread + EPSILON) * column_of(gain_row, channels)
    offset = column_of(shift_row, channels) - mean * slope
    if bias is not None:
        offset = offset + column_of(bias[0][...], channels, bias[1]) * slope
    return jnp.broadcast_to(slope * 0.5, shape), jnp.broadcast_to(offset * 0.5, shape)


def activate(value, coef):
    half = value.astype(F32) * coef[0] + coef[1]
    return (half + half * jnp.tanh(half)).astype(BF16)


def group_stats(sums, squares, bias, channels, pixels, width):
    shape = (channels, LANES)
    lane = lane_index(shape)
    group = group_index(channels, shape)
    inside = lane < width
    mean = jnp.sum(jnp.where(inside, sums, 0.0), axis=1, keepdims=True) * (1.0 / pixels)
    second = jnp.sum(jnp.where(inside, squares, 0.0), axis=1, keepdims=True)
    spread = jnp.maximum(second - pixels * jnp.square(mean), 0.0)
    if bias is not None:
        mean = mean + column_of(bias[0][...], channels, bias[1])
    group_size = channels // GROUPS
    mean_row = jnp.sum(jnp.where(lane == group, mean, 0.0), axis=0, keepdims=True) * (1.0 / group_size)
    group_mean = jnp.sum(jnp.where(lane == group, mean_row, 0.0), axis=1, keepdims=True)
    total = spread + pixels * jnp.square(mean - group_mean)
    return mean_row + jnp.sum(jnp.where(lane == group + GROUPS, total, 0.0), axis=0, keepdims=True)


def frame_rows(taps, first, channels, width, block_rows, rows_of, upper, lower, west, east, place, together=16):
    stride = taps.shape[1] // 3
    lane = lane_index((channels, LANES))
    base = place * block_rows

    def put(row, value, hw, he):
        taps[row, pl.ds(first, channels)] = jnp.where(lane == 0, hw, turn(value, 1))
        taps[row, pl.ds(stride + first, channels)] = value
        taps[row, pl.ds(2 * stride + first, channels)] = jnp.where(lane == width - 1, he, turn(value, LANES - 1))

    def sides(row):
        return turn(west, (LANES - base - row) % LANES), turn(east, (2 * LANES + width - 1 - base - row) % LANES)

    zero = jnp.zeros((channels, LANES), BF16)
    hw, he = sides(-1)
    put(0, upper, jnp.where(place == 0, zero, hw), jnp.where(place == 0, zero, he))

    def body(step, carry):
        for k in range(together):
            row = step * together + k
            put(row + 1, rows_of(row), *sides(row))
        return carry

    lax.fori_loop(0, block_rows // together, body, 0)
    hw, he = sides(block_rows)
    put(block_rows + 1, lower, jnp.where(place == 1, zero, hw), jnp.where(place == 1, zero, he))


def convolve_rows(taps, weight_ref, raw_ref, block_rows, together=16):
    outputs = weight_ref.shape[0]
    depth = taps.shape[1] * 3
    weight = weight_ref[...]
    zero = jnp.zeros((outputs, LANES), F32)

    def body(step, carry):
        sums, squares = carry
        row = step * together
        for k in range(0, together, 2):
            window = jnp.concatenate(
                [taps[pl.ds(row + k + j, 3)].reshape(depth, LANES) for j in range(2)], axis=1
            )
            both = jnp.dot(weight, window, preferred_element_type=F32)
            for j in range(2):
                value = both[:, j * LANES : (j + 1) * LANES]
                raw_ref[row + k + j] = value.astype(BF16)
                sums = sums + value
                squares = squares + value * value
        return sums, squares

    return lax.fori_loop(0, block_rows // together, body, (zero, zero))


def pack_edges(raw_ref, pack_ref, block_rows, channels, width, depth, place, together=16):
    size = depth * channels
    lane = lane_index((channels, LANES))
    last = block_rows - 1
    for d in range(depth):
        outer = jnp.where(place == 0, d, last - d)
        pack_ref[pl.ds(d * channels, channels)] = raw_ref[outer].astype(BF16)
        pack_ref[pl.ds(size + d * channels, channels)] = raw_ref[last - outer].astype(BF16)

    spacing = 2 if width == LANES else 1

    def body(step, carry):
        carry = list(carry)
        for k in range(together):
            row = step * together + k
            value = raw_ref[row].astype(BF16)
            for d in range(depth):
                amount = spacing * row
                west = (lane == amount)
                east = lane == (amount + width - 1) % LANES
                if d:
                    left = turn(value, (amount + LANES - d) % LANES)
                    right = turn(value, (amount + d) % LANES)
                    carry[d] = jnp.where(west, left, jnp.where(east, right, carry[d]))
                else:
                    carry[d] = jnp.where(west | east, turn(value, amount), carry[d])
        return tuple(carry)

    zero = jnp.zeros((channels, LANES), BF16)
    columns = lax.fori_loop(0, block_rows // together, body, (zero,) * depth)
    for d in range(depth):
        pack_ref[pl.ds(2 * size + d * channels, channels)] = columns[d]


def finish(taps, weight_ref, raw_ref, pack_ref, stat_ref, bias, block_rows, channels, width, depth, place):
    sums, squares = convolve_rows(taps, weight_ref, raw_ref, block_rows)
    stat = group_stats(sums, squares, bias, channels, float(block_rows * width), width)
    stat_ref[...] = jnp.broadcast_to(stat, stat_ref.shape)
    if pack_ref is not None:
        pack_edges(raw_ref, pack_ref, block_rows, channels, width, depth, place)


WHOLE = pl.BlockSpec(memory_space=pltpu.VMEM)
SCALARS = pl.BlockSpec(memory_space=pltpu.SMEM)


def call(body, operands, outs, scratch=(), limit=12):
    return pl.pallas_call(
        body,
        in_specs=[SCALARS] + [WHOLE] * (len(operands) - 1),
        out_specs=[WHOLE] * len(outs),
        out_shape=[jax.ShapeDtypeStruct(s, d) for s, d in outs],
        scratch_shapes=list(scratch),
        compiler_params=pltpu.CompilerParams(vmem_limit_bytes=limit * 1024 * 1024),
    )(*operands)


def edges_of_image(here, image, seam_codes):
    block_rows, channels, width = image.shape
    count = seam_codes.shape[0]

    def body(here_ref, codes, image_ref, pack_ref, scalar_ref):
        tile, place = here_ref[0], here_ref[1]
        pack_edges(image_ref, pack_ref, block_rows, channels, width, 1, place)

        def facing(steps, side):
            k = (side + 2 + codes[(tile + count + steps) % count, side]) % 4
            return k, jnp.where((k < 2) == (side < 2), 1, 0)

        odd = tile % 2 == 1
        north, south = facing(ROW_TILES, 0), facing(-ROW_TILES, 2)
        east, west = facing(-1, 1), facing(1, 3)
        scalar_ref[0] = place
        for k in range(2):
            scalar_ref[1 + k] = jnp.where(place == 0, north[k], south[k])
            scalar_ref[3 + k] = jnp.where(odd, east[k], west[k])
            scalar_ref[5 + k] = jnp.where(odd, west[k], east[k])
        scalar_ref[7] = jnp.where(odd, 1, 0)

    return pl.pallas_call(
        body,
        in_specs=[SCALARS, SCALARS, WHOLE],
        out_specs=[WHOLE, SCALARS],
        out_shape=[
            jax.ShapeDtypeStruct((3 * channels, LANES), BF16),
            jax.ShapeDtypeStruct((8,), jnp.int32),
        ],
        compiler_params=pltpu.CompilerParams(vmem_limit_bytes=12 * 1024 * 1024),
    )(here, seam_codes, image)


def strips(scalars, pack, partner, width):
    size = pack.shape[0] // 3
    half = width // 2

    def body(sc, mine_ref, their_ref, ns_ref, near_ref, far_ref, side_ref):
        place = sc[0]
        lane = lane_index((size, LANES))

        def ordered(first):
            mine, theirs = mine_ref[pl.ds(first, size)], their_ref[pl.ds(first, size)]
            return jnp.where(place == 0, mine, theirs), jnp.where(place == 0, theirs, mine)

        low, high = ordered(0)
        side_ref[0] = low
        side_ref[2] = high
        shape = (LANES, LANES)
        row, column = lax.broadcasted_iota(jnp.int32, shape, 0), lane_index(shape)
        low, high = ordered(2 * size)
        both = jnp.concatenate([low, high], axis=1)
        spacing = 2 if width == LANES else 1
        for side, start in ((3, 0), (1, width - 1)):
            upper = (row == (start + spacing * column) % LANES) & (column < half)
            under = (row == (start + spacing * (column - half)) % LANES) & (column >= half) & (column < width)
            spread = jnp.concatenate([upper, under], axis=0)
            spread = jnp.where(spread, 1.0, 0.0).astype(BF16)
            side_ref[side] = jnp.dot(both, spread, preferred_element_type=F32).astype(BF16)
        for k, out in enumerate((ns_ref, near_ref, far_ref)):
            reverse = sc[2 + 2 * k]
            hit = jnp.where(reverse == 1, width - 1 - row, row) == column
            order = jnp.where(hit & (column < width), 1.0, 0.0).astype(BF16)
            strip = jnp.where(lane < width, side_ref[sc[1 + 2 * k]], jnp.zeros((size, LANES), BF16))
            out[...] = jnp.dot(strip, order, preferred_element_type=F32).astype(BF16)

    outs = [((size, LANES), BF16)] * 3
    return call(body, (scalars, pack, partner), outs, [pltpu.VMEM((4, size, LANES), BF16)])


def west_east(scalars, near_ref, far_ref):
    near, far = near_ref[...], far_ref[...]
    odd = scalars[7] == 1
    return jnp.where(odd, near, far), jnp.where(odd, far, near)


def above_below(place, facing, inner):
    return jnp.where(place == 0, facing, inner), jnp.where(place == 0, inner, facing)


def first_stage(scalars, image, partner, ns, near, far, weight, bias):
    block_rows, channels, width = image.shape
    outputs = weight.shape[0]

    def body(sc, image_ref, partner_ref, ns_ref, near_ref, far_ref, weight_ref, bias_ref, raw_ref, pack_ref, stat_ref, taps):
        place = sc[0]
        upper, lower = above_below(place, ns_ref[...], partner_ref[pl.ds(channels, channels)])
        west, east = west_east(sc, near_ref, far_ref)
        frame_rows(taps, 0, channels, width, block_rows, lambda r: image_ref[r], upper, lower, west, east, place)
        finish(taps, weight_ref, raw_ref, pack_ref, stat_ref, (bias_ref, 0), block_rows, outputs, width, 1, place)

    return call(
        body,
        (scalars, image, partner, ns, near, far, weight, bias),
        [((block_rows, outputs, LANES), BF16), ((3 * outputs, LANES), BF16), ((DEVICES, LANES), F32)],
        [pltpu.VMEM((block_rows + 2, 3 * channels, LANES), BF16)],
    )


def plain_stage(scalars, raw, stats, partner, ns, near, far, weight, gain, shift, line, bias, first, width, depth):
    block_rows, channels, _ = raw.shape
    outputs = weight.shape[0]
    biased = bias is not None

    def body(sc, raw_in, stats_ref, partner_ref, ns_ref, near_ref, far_ref, weight_ref, gain_ref, shift_ref, *rest):
        bias_row = None
        if biased:
            bias_row, rest = (rest[0], first), rest[1:]
        if depth:
            raw_ref, stat_ref, pack_ref, taps = rest
        else:
            raw_ref, stat_ref, taps = rest
            pack_ref = None
        place = sc[0]
        coef = coefficients(
            stats_ref[...], gain_ref[line : line + 1], shift_ref[line : line + 1], bias_row, channels, float(block_rows * width)
        )
        lane = lane_index((channels, LANES))
        clear = jnp.zeros((channels, LANES), BF16)

        def strip(value):
            return jnp.where(lane < width, activate(value, coef), clear)

        west, east = west_east(sc, near_ref, far_ref)
        upper, lower = above_below(place, strip(ns_ref[...]), activate(partner_ref[pl.ds(channels, channels)], coef))
        frame_rows(
            taps,
            0,
            channels,
            width,
            block_rows,
            lambda r: activate(raw_in[r], coef),
            upper,
            lower,
            strip(west),
            strip(east),
            place,
        )
        finish(taps, weight_ref, raw_ref, pack_ref, stat_ref, None, block_rows, outputs, width, depth, place)

    outs = [((block_rows, outputs, LANES), BF16), ((DEVICES, LANES), F32)]
    if depth:
        outs.append(((3 * depth * outputs, LANES), BF16))
    operands = (scalars, raw, stats, partner, ns, near, far, weight, gain, shift)
    if biased:
        operands += (bias,)
    return call(body, operands, outs, [pltpu.VMEM((block_rows + 2, 3 * channels, LANES), BF16)])


def pool_stage(scalars, raw, stats, partner, ns, near, far, weight, gain, shift, bias):
    block_rows, channels, width = raw.shape
    low_rows, low_width = block_rows // 2, width // 2
    outputs = weight.shape[0]

    def body(
        sc, raw_in, stats_ref, partner_ref, ns_ref, near_ref, far_ref, weight_ref, gain_ref, shift_ref, bias_ref,
        skip_ref, side_ref, raw_ref, pack_ref, stat_ref, taps, pooled,
    ):
        place = sc[0]
        coef = coefficients(stats_ref[...], gain_ref[1:2], shift_ref[1:2], None, channels, float(block_rows * width))
        shape = (2 * LANES, LANES)
        row, column = lax.broadcasted_iota(jnp.int32, shape, 0), lane_index(shape)
        gather = jnp.where(((row & (LANES - 1)) >> 1) == column, 0.25, 0.0).astype(BF16)

        def pool(outer, second):
            both = jnp.concatenate([outer, second], axis=1)
            return jnp.dot(both, gather, preferred_element_type=F32).astype(BF16)

        def lines(value):
            return activate(value[:channels], coef), activate(value[channels:], coef)

        west, east = west_east(sc, near_ref, far_ref)
        ns_lines, east_lines, west_lines = lines(ns_ref[...]), lines(east), lines(west)
        inner_lines = lines(partner_ref[pl.ds(2 * channels, 2 * channels)])
        upper, lower = above_below(place, ns_lines[0], inner_lines[0])
        side_ref[0] = upper
        side_ref[1] = lower
        side_ref[2] = west_lines[0]
        side_ref[3] = east_lines[0]

        def make(step, carry):
            for k in range(8):
                row = step * 8 + k
                first = activate(raw_in[2 * row], coef)
                second = activate(raw_in[2 * row + 1], coef)
                skip_ref[2 * row] = first
                skip_ref[2 * row + 1] = second
                pooled[row] = pool(first, second)
            return carry

        lax.fori_loop(0, low_rows // 8, make, 0)
        upper, lower = above_below(place, pool(*ns_lines), pool(*inner_lines))
        frame_rows(
            taps,
            0,
            channels,
            low_width,
            low_rows,
            lambda r: pooled[r],
            upper,
            lower,
            pool(*west_lines),
            pool(*east_lines),
            place,
        )
        finish(taps, weight_ref, raw_ref, pack_ref, stat_ref, (bias_ref, channels), low_rows, outputs, low_width, 1, place)

    return call(
        body,
        (scalars, raw, stats, partner, ns, near, far, weight, gain, shift, bias),
        [
            ((block_rows, channels, LANES), BF16),
            ((4, channels, LANES), BF16),
            ((low_rows, outputs, LANES), BF16),
            ((3 * outputs, LANES), BF16),
            ((DEVICES, LANES), F32),
        ],
        [pltpu.VMEM((low_rows + 2, 3 * channels, LANES), BF16), pltpu.VMEM((low_rows, channels, LANES), BF16)],
    )


def decode_stage(scalars, raw, stats, partner, ns, near, far, skip, sides, deep_weight, skip_weight, gain, shift):
    low_rows, channels, _ = raw.shape
    block_rows, skip_channels, width = skip.shape
    low_width = width // 2
    outputs = skip_weight.shape[0]

    def body(
        sc, raw_in, stats_ref, partner_ref, ns_ref, near_ref, far_ref, skip_ref, side_ref, deep_ref, weight_ref, gain_ref,
        shift_ref, raw_ref, pack_ref, stat_ref, deep_taps, skip_taps, wide,
    ):
        place = sc[0]
        coef = coefficients(
            stats_ref[...], gain_ref[1:2], shift_ref[1:2], None, channels, float(low_rows * low_width)
        )
        shape = (LANES, LANES)
        row, column = lax.broadcasted_iota(jnp.int32, shape, 0), lane_index(shape)
        spread = jnp.where(row == column >> 1, 1.0, 0.0).astype(BF16)

        lane = lane_index((channels, LANES))

        def kept(value):
            return jnp.where(lane < low_width, activate(value, coef), jnp.zeros((channels, LANES), BF16))

        def widen(value):
            return jnp.dot(kept(value), spread, preferred_element_type=F32).astype(BF16)

        def make(step, carry):
            for k in range(8):
                wide[step * 8 + k] = widen(raw_in[step * 8 + k])
            return carry

        lax.fori_loop(0, low_rows // 8, make, 0)
        west, east = west_east(sc, near_ref, far_ref)
        upper, lower = above_below(place, widen(ns_ref[...]), widen(partner_ref[pl.ds(channels, channels)]))
        frame_rows(
            deep_taps, 0, channels, width, low_rows, lambda r: wide[r], upper, lower, kept(west), kept(east), place
        )
        frame_rows(
            skip_taps,
            0,
            skip_channels,
            width,
            block_rows,
            lambda r: skip_ref[r],
            side_ref[0],
            side_ref[1],
            side_ref[2],
            side_ref[3],
            place,
        )
        deep_weights, skip_weights = deep_ref[...], weight_ref[...]
        zero = jnp.zeros((outputs, LANES), F32)
        together = 4

        def convolve(step, carry):
            sums, squares = carry
            for k in range(0, together, 2):
                low = step * together + k
                window = jnp.concatenate(
                    [deep_taps[pl.ds(low + j, 3)].reshape(9 * channels, LANES) for j in range(2)], axis=1
                )
                deep = jnp.dot(deep_weights, window, preferred_element_type=F32)
                for j in range(2):
                    high = 2 * (low + j)
                    window = jnp.concatenate(
                        [skip_taps[pl.ds(high + i, 3)].reshape(9 * skip_channels, LANES) for i in range(2)], axis=1
                    )
                    both = jnp.dot(skip_weights, window, preferred_element_type=F32)
                    for i in range(2):
                        value = both[:, i * LANES : (i + 1) * LANES]
                        value = value + deep[i * outputs : (i + 1) * outputs, j * LANES : (j + 1) * LANES]
                        raw_ref[high + i] = value.astype(BF16)
                        sums = sums + value
                        squares = squares + value * value
            return sums, squares

        sums, squares = lax.fori_loop(0, low_rows // together, convolve, (zero, zero))
        stat = group_stats(sums, squares, None, outputs, float(block_rows * width), width)
        stat_ref[...] = jnp.broadcast_to(stat, stat_ref.shape)
        pack_edges(raw_ref, pack_ref, block_rows, outputs, width, 1, place)

    return call(
        body,
        (scalars, raw, stats, partner, ns, near, far, skip, sides, deep_weight, skip_weight, gain, shift),
        [((block_rows, outputs, LANES), BF16), ((3 * outputs, LANES), BF16), ((DEVICES, LANES), F32)],
        [
            pltpu.VMEM((low_rows + 2, 3 * channels, LANES), BF16),
            pltpu.VMEM((block_rows + 2, 3 * skip_channels, LANES), BF16),
            pltpu.VMEM((low_rows, channels, LANES), BF16),
        ],
        16,
    )


def project_stage(scalars, raw, stats, weight, gain, shift, kept):
    block_rows, channels, width = raw.shape

    def body(sc, raw_in, stats_ref, weight_ref, gain_ref, shift_ref, out_ref):
        coef = coefficients(stats_ref[...], gain_ref[3:4], shift_ref[3:4], None, channels, float(block_rows * width))
        project = weight_ref[...]

        def make(step, carry):
            for k in range(0, 16, 2):
                row = step * 16 + k
                both = jnp.concatenate([activate(raw_in[row], coef), activate(raw_in[row + 1], coef)], axis=1)
                result = jnp.dot(project, both, preferred_element_type=F32).astype(BF16)
                out_ref[row] = result[:kept, :LANES]
                out_ref[row + 1] = result[:kept, LANES:]
            return carry

        lax.fori_loop(0, block_rows // 16, make, 0)

    return call(body, (scalars, raw, stats, weight, gain, shift), [((block_rows, kept, LANES), BF16)])[0]


def vertical(value):
    count = lax.axis_size(TILE)
    pairs = []
    for t in range(count):
        pairs.append((2 * t, 2 * ((t + ROW_TILES) % count)))
        pairs.append((2 * t + 1, 2 * ((t - ROW_TILES) % count) + 1))
    return lax.ppermute(value, TILE_SPLIT, pairs)


def exchange(scalars, pack, width):
    partner = lax.ppermute(pack, "split", [(0, 1), (1, 0)])
    ns, near, far = strips(scalars, pack, partner, width)
    count = lax.axis_size(TILE)
    far = lax.ppermute(far, TILE, [(t, (t - 1 + 2 * (t % 2)) % count) for t in range(count)])
    near = lax.ppermute(near, TILE, [(t, t + 1 - 2 * (t % 2)) for t in range(count)])
    ns = vertical(ns)
    return partner, ns, near, far


def share(stat):
    copies = stat.reshape(DEVICES, 1, LANES)
    return lax.all_to_all(copies, TILE_SPLIT, 0, 0).reshape(DEVICES, LANES)


def meet(scalars, pack, stat, width):
    received = exchange(scalars, pack, width) if pack is not None else None
    return (share(stat) if stat is not None else None), received


def embedding(timestep, time_weight, bias_upper, bias_lower):
    moment = timestep[0].astype(F32)
    half_width = time_weight.shape[0] // 2
    frequencies = jnp.exp(-math.log(10000.0) * jnp.arange(half_width, dtype=F32) / half_width)
    angles = moment * frequencies
    features = jnp.concatenate([jnp.sin(angles), jnp.cos(angles)])[None, :]
    embedded = jax.nn.silu(jnp.dot(features, time_weight, precision=lax.Precision.HIGHEST))
    both = jnp.concatenate([bias_upper, bias_lower], axis=1)
    biases = jnp.dot(embedded, both, precision=lax.Precision.HIGHEST)
    return biases


def flat_kernel(kernel):
    return jnp.transpose(kernel, (2, 0, 1, 3)).reshape(kernel.shape[2], -1)


def deep_kernel(kernel):
    wide = kernel.astype(F32)
    none = jnp.zeros_like(wide[0])
    even = jnp.stack([wide[0], wide[1] + wide[2], none])
    odd = jnp.stack([none, wide[0] + wide[1], wide[2]])
    both = jnp.stack([even, odd]).astype(BF16)
    return jnp.transpose(both, (0, 3, 1, 2, 4)).reshape(2 * kernel.shape[2], -1)


def per_device(
    noisy_image,
    seam_codes,
    timestep,
    time_weight,
    bias_upper,
    bias_lower,
    kernel_upper_first,
    kernel_upper_second,
    kernel_lower_first,
    kernel_lower_second,
    kernel_decode_first,
    kernel_decode_second,
    output_weight,
    gains_upper,
    shifts_upper,
    gains_lower,
    shifts_lower,
):
    here = jnp.stack([lax.axis_index(TILE), lax.axis_index("split")]).astype(jnp.int32)
    biases = embedding(timestep, time_weight, bias_upper, bias_lower)
    channels, _, width = noisy_image.shape[1:]
    padding = kernel_upper_first.shape[2] - channels
    image = jnp.transpose(jnp.pad(noisy_image[0], ((0, padding), (0, 0), (0, 0))), (1, 0, 2))
    upper_first = flat_kernel(jnp.pad(kernel_upper_first, ((0, 0), (0, 0), (0, 0), (0, padding))))
    low_width = width // 2
    width_one = kernel_upper_first.shape[2]

    pack, scalars = edges_of_image(here, image, seam_codes)
    _, received = meet(scalars, pack, None, width)
    raw, pack, stat = first_stage(scalars, image, *received, upper_first, biases)

    stats, received = meet(scalars, pack, stat, width)
    raw, stat, pack = plain_stage(
        scalars, raw, stats, *received, flat_kernel(kernel_upper_second), gains_upper, shifts_upper, 0, biases, 0, width, 2
    )

    stats, received = meet(scalars, pack, stat, width)
    skip, sides, raw, pack, stat = pool_stage(
        scalars, raw, stats, *received, flat_kernel(kernel_lower_first), gains_upper, shifts_upper, biases
    )

    stats, received = meet(scalars, pack, stat, low_width)
    raw, stat, pack = plain_stage(
        scalars, raw, stats, *received, flat_kernel(kernel_lower_second), gains_lower, shifts_lower, 0, biases, width_one,
        low_width, 1,
    )

    stats, received = meet(scalars, pack, stat, low_width)
    raw, pack, stat = decode_stage(
        scalars, raw, stats, *received, skip, sides, deep_kernel(kernel_decode_first[..., :-width_one]),
        flat_kernel(kernel_decode_first[..., -width_one:]), gains_lower, shifts_lower,
    )

    stats, received = meet(scalars, pack, stat, width)
    raw, stat = plain_stage(
        scalars, raw, stats, *received, flat_kernel(kernel_decode_second), gains_upper, shifts_upper, 2, None, 0, width, 0
    )

    stats, _ = meet(scalars, None, stat, width)
    project = jnp.pad(output_weight, ((0, padding), (0, 0)))
    result = project_stage(scalars, raw, stats, project, gains_upper, shifts_upper, channels)
    return jnp.transpose(result, (1, 0, 2))[None]


def solution(mesh):
    torus = Mesh(
        mesh.devices.reshape(4, 4, 2, 2, mesh.shape["split"]),
        ("tile_0", "tile_1", "tile_2", "tile_3", "split"),
    )
    return jax.shard_map(
        per_device,
        mesh=torus,
        in_specs=(P(TILE, None, "split", None),) + (P(),) * 16,
        out_specs=P(TILE, None, "split", None),
        check_vma=False,
    )
```

```python
import math

import jax
import jax.numpy as jnp
from jax import lax
from jax.experimental import pallas as pl
from jax.experimental.pallas import tpu as pltpu
from jax.sharding import Mesh
from jax.sharding import PartitionSpec as P


GROUPS = 8
ROW_TILES = 4
TILE = ("tile_0", "tile_1", "tile_2", "tile_3")
TILE_SPLIT = ("tile_0", "tile_1", "tile_2", "tile_3", "split")
EPSILON = 1e-05
LANES = 128
DEVICES = 128
TOGETHER = 64
F32 = jnp.float32
BF16 = jnp.bfloat16


def lane_index(shape):
    return lax.broadcasted_iota(jnp.int32, shape, 1)


def turn(value, amount):
    return pltpu.roll(value, amount, 1)


def group_index(channels, shape):
    row = lax.broadcasted_iota(jnp.int32, shape, 0)
    return (row * 43) >> (8 if channels == 48 else 9)


def column_of(row_value, channels, first=0):
    shape = (channels, row_value.shape[1])
    on_diagonal = lax.broadcasted_iota(jnp.int32, shape, 0) + first == lane_index(shape)
    return jnp.sum(jnp.where(on_diagonal, jnp.broadcast_to(row_value, shape), 0.0), axis=1, keepdims=True)


def coefficients(stats, gain_row, shift_row, bias, channels, pixels):
    devices = stats.shape[0]
    count = pixels * (channels // GROUPS)
    mean_row = jnp.sum(stats, axis=0, keepdims=True) * (1.0 / devices)
    apart = jnp.sum(jnp.square(stats - mean_row), axis=0, keepdims=True) * (1.0 / devices)
    shape = (channels, LANES)
    group = group_index(channels, shape)
    lane = lane_index(shape)

    def pick(row_value, first):
        return jnp.sum(jnp.where(lane == group + first, jnp.broadcast_to(row_value, shape), 0.0), axis=1, keepdims=True)

    mean = pick(mean_row, 0)
    spread = pick(mean_row, GROUPS) * (1.0 / count) + pick(apart, 0)
    slope = lax.rsqrt(spread + EPSILON) * column_of(gain_row, channels)
    offset = column_of(shift_row, channels) - mean * slope
    if bias is not None:
        offset = offset + column_of(bias[0][...], channels, bias[1]) * slope
    return jnp.broadcast_to(slope * 0.5, shape), jnp.broadcast_to(offset * 0.5, shape)


def activate(value, coef):
    half = value.astype(F32) * coef[0] + coef[1]
    return (half + half * jnp.tanh(half)).astype(BF16)


def group_stats(sums, squares, bias, channels, pixels, width):
    shape = (channels, LANES)
    lane = lane_index(shape)
    group = group_index(channels, shape)
    inside = lane < width
    mean = jnp.sum(jnp.where(inside, sums, 0.0), axis=1, keepdims=True) * (1.0 / pixels)
    second = jnp.sum(jnp.where(inside, squares, 0.0), axis=1, keepdims=True)
    spread = jnp.maximum(second - pixels * jnp.square(mean), 0.0)
    if bias is not None:
        mean = mean + column_of(bias[0][...], channels, bias[1])
    group_size = channels // GROUPS
    mean_row = jnp.sum(jnp.where(lane == group, mean, 0.0), axis=0, keepdims=True) * (1.0 / group_size)
    group_mean = jnp.sum(jnp.where(lane == group, mean_row, 0.0), axis=1, keepdims=True)
    total = spread + pixels * jnp.square(mean - group_mean)
    return mean_row + jnp.sum(jnp.where(lane == group + GROUPS, total, 0.0), axis=0, keepdims=True)


def frame_rows(taps, first, channels, width, block_rows, rows_of, upper, lower, west, east, place):
    stride = taps.shape[1] // 3
    together = min(block_rows, TOGETHER)
    lane = lane_index((channels, LANES))
    base = place * block_rows

    def put(row, value, hw, he):
        taps[row, pl.ds(first, channels)] = jnp.where(lane == 0, hw, turn(value, 1))
        taps[row, pl.ds(stride + first, channels)] = value
        taps[row, pl.ds(2 * stride + first, channels)] = jnp.where(lane == width - 1, he, turn(value, LANES - 1))

    def sides(row):
        return turn(west, (LANES - base - row) % LANES), turn(east, (2 * LANES + width - 1 - base - row) % LANES)

    zero = jnp.zeros((channels, LANES), BF16)
    hw, he = sides(-1)
    put(0, upper, jnp.where(place == 0, zero, hw), jnp.where(place == 0, zero, he))

    def body(step, carry):
        for k in range(together):
            row = step * together + k
            put(row + 1, rows_of(row), *sides(row))
        return carry

    lax.fori_loop(0, block_rows // together, body, 0)
    hw, he = sides(block_rows)
    put(block_rows + 1, lower, jnp.where(place == 1, zero, hw), jnp.where(place == 1, zero, he))


def convolve_rows(taps, weight_ref, raw_ref, block_rows):
    outputs = weight_ref.shape[0]
    together = min(block_rows, TOGETHER)
    depth = taps.shape[1] * 3
    weight = weight_ref[...]
    zero = jnp.zeros((outputs, LANES), F32)

    def body(step, carry):
        sums, squares = carry
        row = step * together
        for k in range(0, together, 2):
            window = jnp.concatenate(
                [taps[pl.ds(row + k + j, 3)].reshape(depth, LANES) for j in range(2)], axis=1
            )
            both = jnp.dot(weight, window, preferred_element_type=F32)
            for j in range(2):
                value = both[:, j * LANES : (j + 1) * LANES]
                raw_ref[row + k + j] = value.astype(raw_ref.dtype)
                sums = sums + value
                squares = squares + value * value
        return sums, squares

    return lax.fori_loop(0, block_rows // together, body, (zero, zero))


def pack_edges(raw_ref, pack_ref, block_rows, channels, width, depth, place):
    size = depth * channels
    together = min(block_rows, TOGETHER)
    lane = lane_index((channels, LANES))
    last = block_rows - 1
    for d in range(depth):
        outer = jnp.where(place == 0, d, last - d)
        pack_ref[pl.ds(d * channels, channels)] = raw_ref[outer].astype(BF16)
        pack_ref[pl.ds(size + d * channels, channels)] = raw_ref[last - outer].astype(BF16)

    spacing = 2 if width == LANES else 1

    def body(step, carry):
        carry = list(carry)
        for k in range(together):
            row = step * together + k
            value = raw_ref[row].astype(BF16)
            for d in range(depth):
                amount = spacing * row
                west = (lane == amount)
                east = lane == (amount + width - 1) % LANES
                if d:
                    left = turn(value, (amount + LANES - d) % LANES)
                    right = turn(value, (amount + d) % LANES)
                    carry[d] = jnp.where(west, left, jnp.where(east, right, carry[d]))
                else:
                    carry[d] = jnp.where(west | east, turn(value, amount), carry[d])
        return tuple(carry)

    zero = jnp.zeros((channels, LANES), BF16)
    columns = lax.fori_loop(0, block_rows // together, body, (zero,) * depth)
    for d in range(depth):
        pack_ref[pl.ds(2 * size + d * channels, channels)] = columns[d]


def send_stats(stat, held, stat_ref, sent):
    held[...] = jnp.broadcast_to(stat, held.shape)
    leave = pltpu.make_async_copy(held, stat_ref, sent)
    leave.start()
    return leave


def finish(taps, weight_ref, raw_ref, pack_ref, stat_ref, held, sent, bias, block_rows, channels, width, depth, place):
    sums, squares = convolve_rows(taps, weight_ref, raw_ref, block_rows)
    stat = group_stats(sums, squares, bias, channels, float(block_rows * width), width)
    leave = send_stats(stat, held, stat_ref, sent)
    if pack_ref is not None:
        pack_edges(raw_ref, pack_ref, block_rows, channels, width, depth, place)
    leave.wait()


WHOLE = pl.BlockSpec(memory_space=pltpu.VMEM)
SCALARS = pl.BlockSpec(memory_space=pltpu.SMEM)
ANYWHERE = pl.BlockSpec(memory_space=pl.ANY)
STATS = (pltpu.VMEM((DEVICES, LANES), F32), pltpu.SemaphoreType.DMA)


def call(body, operands, outs, scratch=(), limit=12):
    return pl.pallas_call(
        body,
        in_specs=[SCALARS] + [WHOLE] * (len(operands) - 1),
        out_specs=[ANYWHERE if s == (DEVICES, LANES) else WHOLE for s, _ in outs],
        out_shape=[jax.ShapeDtypeStruct(s, d) for s, d in outs],
        scratch_shapes=list(scratch),
        compiler_params=pltpu.CompilerParams(vmem_limit_bytes=limit * 1024 * 1024),
    )(*operands)


def edges_of_image(here, image):
    block_rows, channels, width = image.shape

    def body(here_ref, image_ref, pack_ref):
        pack_edges(image_ref, pack_ref, block_rows, channels, width, 1, here_ref[1])

    return call(body, (here, image), [((3 * channels, LANES), BF16)])[0]


def setup(here, seam_codes, tables):
    count = seam_codes.shape[0]

    def body(here_ref, codes, *rest):
        table_refs, (scalar_ref, param_ref) = rest[: len(tables)], rest[len(tables) :]
        tile, place = here_ref[0], here_ref[1]
        for k, table_ref in enumerate(table_refs):
            lines, columns = table_ref.shape
            param_ref[4 * k : 4 * k + lines, 0:columns] = table_ref[...]

        def facing(steps, side):
            k = (side + 2 + codes[(tile + count + steps) % count, side]) % 4
            return k, jnp.where((k < 2) == (side < 2), 1, 0)

        odd = tile % 2 == 1
        north, south = facing(ROW_TILES, 0), facing(-ROW_TILES, 2)
        east, west = facing(-1, 1), facing(1, 3)
        scalar_ref[0] = place
        for k in range(2):
            scalar_ref[1 + k] = jnp.where(place == 0, north[k], south[k])
            scalar_ref[3 + k] = jnp.where(odd, east[k], west[k])
            scalar_ref[5 + k] = jnp.where(odd, west[k], east[k])
        scalar_ref[7] = jnp.where(odd, 1, 0)

    return pl.pallas_call(
        body,
        in_specs=[SCALARS, SCALARS] + [WHOLE] * len(tables),
        out_specs=[SCALARS, WHOLE],
        out_shape=[
            jax.ShapeDtypeStruct((8,), jnp.int32),
            jax.ShapeDtypeStruct((4 * len(tables), LANES), F32),
        ],
        compiler_params=pltpu.CompilerParams(vmem_limit_bytes=2 * 1024 * 1024),
    )(here, seam_codes, *tables)


def strips(scalars, pack, partner, width):
    size = pack.shape[0] // 3
    half = width // 2

    def body(sc, mine_ref, their_ref, ns_ref, near_ref, far_ref, side_ref):
        place = sc[0]
        lane = lane_index((size, LANES))

        def ordered(first):
            mine, theirs = mine_ref[pl.ds(first, size)], their_ref[pl.ds(first, size)]
            return jnp.where(place == 0, mine, theirs), jnp.where(place == 0, theirs, mine)

        low, high = ordered(0)
        side_ref[0] = low
        side_ref[2] = high
        shape = (LANES, LANES)
        row, column = lax.broadcasted_iota(jnp.int32, shape, 0), lane_index(shape)
        low, high = ordered(2 * size)
        both = jnp.concatenate([low, high], axis=1)
        spacing = 2 if width == LANES else 1
        for side, start in ((3, 0), (1, width - 1)):
            upper = (row == (start + spacing * column) % LANES) & (column < half)
            under = (row == (start + spacing * (column - half)) % LANES) & (column >= half) & (column < width)
            spread = jnp.concatenate([upper, under], axis=0)
            spread = jnp.where(spread, 1.0, 0.0).astype(BF16)
            side_ref[side] = jnp.dot(both, spread, preferred_element_type=F32).astype(BF16)
        for k, out in enumerate((ns_ref, near_ref, far_ref)):
            reverse = sc[2 + 2 * k]
            hit = jnp.where(reverse == 1, width - 1 - row, row) == column
            order = jnp.where(hit & (column < width), 1.0, 0.0).astype(BF16)
            strip = jnp.where(lane < width, side_ref[sc[1 + 2 * k]], jnp.zeros((size, LANES), BF16))
            out[...] = jnp.dot(strip, order, preferred_element_type=F32).astype(BF16)

    outs = [((size, LANES), BF16)] * 3
    return call(body, (scalars, pack, partner), outs, [pltpu.VMEM((4, size, LANES), BF16)])


def norm_lines(param_ref, line):
    return param_ref[line : line + 1], param_ref[line + 4 : line + 5]


def west_east(scalars, near_ref, far_ref):
    near, far = near_ref[...], far_ref[...]
    odd = scalars[7] == 1
    return jnp.where(odd, near, far), jnp.where(odd, far, near)


def above_below(place, facing, inner):
    return jnp.where(place == 0, facing, inner), jnp.where(place == 0, inner, facing)


def first_stage(scalars, image, partner, ns, near, far, weight, bias):
    block_rows, channels, width = image.shape
    outputs = weight.shape[0]

    def body(sc, image_ref, partner_ref, ns_ref, near_ref, far_ref, weight_ref, bias_ref, *rest):
        raw_ref, pack_ref, stat_ref, taps, held, sent = rest
        place = sc[0]
        upper, lower = above_below(place, ns_ref[...], partner_ref[pl.ds(channels, channels)])
        west, east = west_east(sc, near_ref, far_ref)
        frame_rows(taps, 0, channels, width, block_rows, lambda r: image_ref[r], upper, lower, west, east, place)
        finish(taps, weight_ref, raw_ref, pack_ref, stat_ref, held, sent, (bias_ref, 0), block_rows, outputs, width, 1, place)

    return call(
        body,
        (scalars, image, partner, ns, near, far, weight, bias),
        [
            ((block_rows, outputs, LANES), BF16),
            ((3 * outputs, LANES), BF16),
            ((DEVICES, LANES), F32),
        ],
        [pltpu.VMEM((block_rows + 2, 3 * channels, LANES), BF16), *STATS],
    )


def plain_stage(scalars, raw, stats, partner, ns, near, far, weight, params, line, bias, first, width, depth):
    block_rows, channels, _ = raw.shape
    outputs = weight.shape[0]
    biased = bias is not None

    def body(sc, raw_in, stats_ref, partner_ref, ns_ref, near_ref, far_ref, weight_ref, param_ref, *rest):
        bias_row = None
        if biased:
            bias_row, rest = (rest[0], first), rest[1:]
        if depth:
            raw_ref, stat_ref, pack_ref, taps, held, sent = rest
        else:
            raw_ref, stat_ref, taps, held, sent = rest
            pack_ref = None
        place = sc[0]
        coef = coefficients(
            stats_ref[...], *norm_lines(param_ref, line), bias_row, channels, float(block_rows * width)
        )
        lane = lane_index((channels, LANES))
        clear = jnp.zeros((channels, LANES), BF16)

        def strip(value):
            return jnp.where(lane < width, activate(value, coef), clear)

        west, east = west_east(sc, near_ref, far_ref)
        upper, lower = above_below(place, strip(ns_ref[...]), activate(partner_ref[pl.ds(channels, channels)], coef))
        frame_rows(
            taps,
            0,
            channels,
            width,
            block_rows,
            lambda r: activate(raw_in[r], coef),
            upper,
            lower,
            strip(west),
            strip(east),
            place,
        )
        finish(
            taps, weight_ref, raw_ref, pack_ref, stat_ref, held, sent, None, block_rows, outputs, width, depth, place
        )

    outs = [((block_rows, outputs, LANES), BF16), ((DEVICES, LANES), F32)]
    if depth:
        outs.append(((3 * depth * outputs, LANES), BF16))
    operands = (scalars, raw, stats, partner, ns, near, far, weight, params)
    if biased:
        operands += (bias,)
    return call(body, operands, outs, [pltpu.VMEM((block_rows + 2, 3 * channels, LANES), BF16), *STATS])


def pool_stage(scalars, raw, stats, partner, ns, near, far, weight, params, bias):
    block_rows, channels, width = raw.shape
    low_rows, low_width = block_rows // 2, width // 2
    outputs = weight.shape[0]

    def body(
        sc, raw_in, stats_ref, partner_ref, ns_ref, near_ref, far_ref, weight_ref, param_ref, bias_ref,
        skip_ref, side_ref, raw_ref, pack_ref, stat_ref, taps, pooled, held, sent,
    ):
        place = sc[0]
        coef = coefficients(stats_ref[...], *norm_lines(param_ref, 1), None, channels, float(block_rows * width))
        shape = (2 * LANES, LANES)
        row, column = lax.broadcasted_iota(jnp.int32, shape, 0), lane_index(shape)
        gather = jnp.where(((row & (LANES - 1)) >> 1) == column, 0.25, 0.0).astype(BF16)

        def pool(outer, second):
            both = jnp.concatenate([outer, second], axis=1)
            return jnp.dot(both, gather, preferred_element_type=F32).astype(BF16)

        def lines(value):
            return activate(value[:channels], coef), activate(value[channels:], coef)

        west, east = west_east(sc, near_ref, far_ref)
        ns_lines, east_lines, west_lines = lines(ns_ref[...]), lines(east), lines(west)
        inner_lines = lines(partner_ref[pl.ds(2 * channels, 2 * channels)])
        upper, lower = above_below(place, ns_lines[0], inner_lines[0])
        side_ref[0] = upper
        side_ref[1] = lower
        side_ref[2] = west_lines[0]
        side_ref[3] = east_lines[0]

        def make(step, carry):
            for k in range(low_rows):
                row = step * low_rows + k
                first = activate(raw_in[2 * row], coef)
                second = activate(raw_in[2 * row + 1], coef)
                skip_ref[2 * row] = first
                skip_ref[2 * row + 1] = second
                pooled[row] = pool(first, second)
            return carry

        lax.fori_loop(0, 1, make, 0)
        upper, lower = above_below(place, pool(*ns_lines), pool(*inner_lines))
        frame_rows(
            taps,
            0,
            channels,
            low_width,
            low_rows,
            lambda r: pooled[r],
            upper,
            lower,
            pool(*west_lines),
            pool(*east_lines),
            place,
        )
        finish(taps, weight_ref, raw_ref, pack_ref, stat_ref, held, sent, (bias_ref, channels), low_rows, outputs, low_width, 1, place)

    return call(
        body,
        (scalars, raw, stats, partner, ns, near, far, weight, params, bias),
        [
            ((block_rows, channels, LANES), BF16),
            ((4, channels, LANES), BF16),
            ((low_rows, outputs, LANES), BF16),
            ((3 * outputs, LANES), BF16),
            ((DEVICES, LANES), F32),
        ],
        [
            pltpu.VMEM((low_rows + 2, 3 * channels, LANES), BF16),
            pltpu.VMEM((low_rows, channels, LANES), BF16),
            *STATS,
        ],
    )


def skip_stage(scalars, skip, sides, weight):
    block_rows, channels, width = skip.shape
    outputs = weight.shape[0]

    def body(sc, skip_ref, side_ref, weight_ref, part_ref, taps):
        frame_rows(
            taps,
            0,
            channels,
            width,
            block_rows,
            lambda r: skip_ref[r],
            side_ref[0],
            side_ref[1],
            side_ref[2],
            side_ref[3],
            sc[0],
        )
        convolve_rows(taps, weight_ref, part_ref, block_rows)

    return call(
        body,
        (scalars, skip, sides, weight),
        [((block_rows, outputs, LANES), BF16)],
        [pltpu.VMEM((block_rows + 2, 3 * channels, LANES), BF16)],
    )[0]


def decode_stage(scalars, raw, stats, partner, ns, near, far, part, deep_weight, params):
    low_rows, channels, _ = raw.shape
    block_rows, outputs, width = part.shape
    low_width = width // 2

    def body(
        sc, raw_in, stats_ref, partner_ref, ns_ref, near_ref, far_ref, part_ref, deep_ref, param_ref,
        raw_ref, pack_ref, stat_ref, deep_taps, wide, held, sent,
    ):
        place = sc[0]
        coef = coefficients(
            stats_ref[...], *norm_lines(param_ref, 9), None, channels, float(low_rows * low_width)
        )
        shape = (LANES, LANES)
        row, column = lax.broadcasted_iota(jnp.int32, shape, 0), lane_index(shape)
        spread = jnp.where(row == column >> 1, 1.0, 0.0).astype(BF16)

        lane = lane_index((channels, LANES))

        def kept(value):
            return jnp.where(lane < low_width, activate(value, coef), jnp.zeros((channels, LANES), BF16))

        def widen(value):
            return jnp.dot(kept(value), spread, preferred_element_type=F32).astype(BF16)

        def make(step, carry):
            for k in range(low_rows):
                wide[step * low_rows + k] = widen(raw_in[step * low_rows + k])
            return carry

        lax.fori_loop(0, 1, make, 0)
        west, east = west_east(sc, near_ref, far_ref)
        upper, lower = above_below(place, widen(ns_ref[...]), widen(partner_ref[pl.ds(channels, channels)]))
        frame_rows(
            deep_taps, 0, channels, width, low_rows, lambda r: wide[r], upper, lower, kept(west), kept(east), place
        )
        deep_weights = deep_ref[...]
        zero = jnp.zeros((outputs, LANES), F32)
        together = 32

        def convolve(step, carry):
            sums, squares = carry
            for k in range(0, together, 2):
                low = step * together + k
                window = jnp.concatenate(
                    [deep_taps[pl.ds(low + j, 3)].reshape(9 * channels, LANES) for j in range(2)], axis=1
                )
                deep = jnp.dot(deep_weights, window, preferred_element_type=F32)
                for j in range(2):
                    high = 2 * (low + j)
                    for i in range(2):
                        value = part_ref[high + i].astype(F32)
                        value = value + deep[i * outputs : (i + 1) * outputs, j * LANES : (j + 1) * LANES]
                        raw_ref[high + i] = value.astype(BF16)
                        sums = sums + value
                        squares = squares + value * value
            return sums, squares

        sums, squares = lax.fori_loop(0, low_rows // together, convolve, (zero, zero))
        stat = group_stats(sums, squares, None, outputs, float(block_rows * width), width)
        leave = send_stats(stat, held, stat_ref, sent)
        pack_edges(raw_ref, pack_ref, block_rows, outputs, width, 1, place)
        leave.wait()

    return call(
        body,
        (scalars, raw, stats, partner, ns, near, far, part, deep_weight, params),
        [((block_rows, outputs, LANES), BF16), ((3 * outputs, LANES), BF16), ((DEVICES, LANES), F32)],
        [
            pltpu.VMEM((low_rows + 2, 3 * channels, LANES), BF16),
            pltpu.VMEM((low_rows, channels, LANES), BF16),
            *STATS,
        ],
    )


def project_stage(scalars, raw, stats, weight, params, kept):
    block_rows, channels, width = raw.shape

    def body(sc, raw_in, stats_ref, weight_ref, param_ref, out_ref):
        coef = coefficients(stats_ref[...], *norm_lines(param_ref, 3), None, channels, float(block_rows * width))
        project = weight_ref[...]

        def make(step, carry):
            for k in range(0, 64, 2):
                row = step * 64 + k
                both = jnp.concatenate([activate(raw_in[row], coef), activate(raw_in[row + 1], coef)], axis=1)
                result = jnp.dot(project, both, preferred_element_type=F32).astype(BF16)
                out_ref[row] = result[:kept, :LANES]
                out_ref[row + 1] = result[:kept, LANES:]
            return carry

        lax.fori_loop(0, block_rows // 64, make, 0)

    return call(body, (scalars, raw, stats, weight, params), [((block_rows, kept, LANES), BF16)])[0]


def vertical(value):
    count = lax.axis_size(TILE)
    pairs = []
    for t in range(count):
        pairs.append((2 * t, 2 * ((t + ROW_TILES) % count)))
        pairs.append((2 * t + 1, 2 * ((t - ROW_TILES) % count) + 1))
    return lax.ppermute(value, TILE_SPLIT, pairs)


def exchange(scalars, pack, width, later=()):
    partner = lax.ppermute(pack, "split", [(0, 1), (1, 0)])
    ns, near, far = strips(scalars, pack, partner, width)
    (ns, near, far), later = lax.optimization_barrier(((ns, near, far), later)) if later else ((ns, near, far), later)
    count = lax.axis_size(TILE)
    far = lax.ppermute(far, TILE, [(t, (t - 1 + 2 * (t % 2)) % count) for t in range(count)])
    near = lax.ppermute(near, TILE, [(t, t + 1 - 2 * (t % 2)) for t in range(count)])
    ns = vertical(ns)
    return (partner, ns, near, far), later


def share(stat):
    copies = stat.reshape(DEVICES, 1, LANES)
    return lax.all_to_all(copies, TILE_SPLIT, 0, 0).reshape(DEVICES, LANES)


def meet(scalars, pack, stat, width):
    received = exchange(scalars, pack, width)[0] if pack is not None else None
    return (share(stat) if stat is not None else None), received


def embedding(timestep, time_weight, bias_upper, bias_lower):
    moment = timestep[0].astype(F32)
    half_width = time_weight.shape[0] // 2
    frequencies = jnp.exp(-math.log(10000.0) * jnp.arange(half_width, dtype=F32) / half_width)
    angles = moment * frequencies
    features = jnp.concatenate([jnp.sin(angles), jnp.cos(angles)])[None, :]
    embedded = jax.nn.silu(jnp.dot(features, time_weight, precision=lax.Precision.HIGHEST))
    both = jnp.concatenate([bias_upper, bias_lower], axis=1)
    biases = jnp.dot(embedded, both, precision=lax.Precision.HIGHEST)
    return biases


def flat_kernel(kernel):
    return jnp.transpose(kernel, (2, 0, 1, 3)).reshape(kernel.shape[2], -1)


def deep_kernel(kernel):
    wide = kernel.astype(F32)
    none = jnp.zeros_like(wide[0])
    even = jnp.stack([wide[0], wide[1] + wide[2], none])
    odd = jnp.stack([none, wide[0] + wide[1], wide[2]])
    both = jnp.stack([even, odd]).astype(BF16)
    return jnp.transpose(both, (0, 3, 1, 2, 4)).reshape(2 * kernel.shape[2], -1)


def per_device(
    noisy_image,
    seam_codes,
    timestep,
    time_weight,
    bias_upper,
    bias_lower,
    kernel_upper_first,
    kernel_upper_second,
    kernel_lower_first,
    kernel_lower_second,
    kernel_decode_first,
    kernel_decode_second,
    output_weight,
    gains_upper,
    shifts_upper,
    gains_lower,
    shifts_lower,
):
    here = jnp.stack([lax.axis_index(TILE), lax.axis_index("split")]).astype(jnp.int32)
    channels, _, width = noisy_image.shape[1:]
    padding = kernel_upper_first.shape[2] - channels
    image = jnp.transpose(jnp.pad(noisy_image[0], ((0, padding), (0, 0), (0, 0))), (1, 0, 2))
    low_width = width // 2
    width_one = kernel_upper_first.shape[2]

    pack = edges_of_image(here, image)
    scalars, params = setup(here, seam_codes, (gains_upper, shifts_upper, gains_lower, shifts_lower))
    received, prepared = exchange(
        scalars,
        pack,
        width,
        (
            timestep,
            time_weight,
            bias_upper,
            bias_lower,
            kernel_upper_first,
            kernel_upper_second,
            kernel_lower_first,
            kernel_lower_second,
            kernel_decode_first,
            kernel_decode_second,
            output_weight,
        ),
    )
    timestep, time_weight, bias_upper, bias_lower, kernel_upper_first, kernel_upper_second = prepared[:6]
    kernel_lower_first, kernel_lower_second, kernel_decode_first, kernel_decode_second, output_weight = prepared[6:]
    biases = embedding(timestep, time_weight, bias_upper, bias_lower)
    weights = (
        flat_kernel(jnp.pad(kernel_upper_first, ((0, 0), (0, 0), (0, 0), (0, padding)))),
        flat_kernel(kernel_upper_second),
        flat_kernel(kernel_lower_first),
        flat_kernel(kernel_lower_second),
        flat_kernel(kernel_decode_first[..., -width_one:]),
        deep_kernel(kernel_decode_first[..., :-width_one]),
        flat_kernel(kernel_decode_second),
        jnp.pad(output_weight, ((0, padding), (0, 0))),
        biases,
    )
    received, weights = lax.optimization_barrier((received, weights))
    upper_first, upper_second, lower_first, lower_second, decode_skip, decode_deep, decode_second, project, biases = weights
    raw, pack, stat = first_stage(scalars, image, *received, upper_first, biases)

    stats, received = meet(scalars, pack, stat, width)
    raw, stat, pack = plain_stage(
        scalars, raw, stats, *received, upper_second, params, 0, biases, 0, width, 2
    )

    stats, received = meet(scalars, pack, stat, width)
    skip, sides, raw, pack, stat = pool_stage(
        scalars, raw, stats, *received, lower_first, params, biases
    )

    stats, received = meet(scalars, pack, stat, low_width)
    part = skip_stage(scalars, skip, sides, decode_skip)
    raw, stat, pack = plain_stage(
        scalars, raw, stats, *received, lower_second, params, 8, biases, width_one,
        low_width, 1,
    )

    stats, received = meet(scalars, pack, stat, low_width)
    raw, pack, stat = decode_stage(
        scalars, raw, stats, *received, part, decode_deep, params
    )

    stats, received = meet(scalars, pack, stat, width)
    raw, stat = plain_stage(
        scalars, raw, stats, *received, decode_second, params, 2, None, 0, width, 0
    )

    stats, _ = meet(scalars, None, stat, width)
    result = project_stage(scalars, raw, stats, project, params, channels)
    return jnp.transpose(result, (1, 0, 2))[None]


def solution(mesh):
    torus = Mesh(
        mesh.devices.reshape(4, 4, 2, 2, mesh.shape["split"]),
        ("tile_0", "tile_1", "tile_2", "tile_3", "split"),
    )
    return jax.shard_map(
        per_device,
        mesh=torus,
        in_specs=(P(TILE, None, "split", None),) + (P(),) * 16,
        out_specs=P(TILE, None, "split", None),
        check_vma=False,
    )
```

```python
import math

import jax
import jax.numpy as jnp
from jax import lax
from jax.experimental import pallas as pl
from jax.experimental.pallas import tpu as pltpu
from jax.sharding import Mesh
from jax.sharding import PartitionSpec as P


GROUPS = 8
ROW_TILES = 4
TILE = ("tile_0", "tile_1", "tile_2", "tile_3")
TILE_SPLIT = ("tile_0", "tile_1", "tile_2", "tile_3", "split")
EPSILON = 1e-05
LANES = 128
DEVICES = 128
TOGETHER = 64
F32 = jnp.float32
BF16 = jnp.bfloat16


def lane_index(shape):
    return lax.broadcasted_iota(jnp.int32, shape, 1)


def turn(value, amount):
    return pltpu.roll(value, amount, 1)


def group_index(channels, shape):
    row = lax.broadcasted_iota(jnp.int32, shape, 0)
    return (row * 43) >> (8 if channels == 48 else 9)


def column_of(row_value, channels, first=0):
    shape = (channels, row_value.shape[1])
    on_diagonal = lax.broadcasted_iota(jnp.int32, shape, 0) + first == lane_index(shape)
    return jnp.sum(jnp.where(on_diagonal, jnp.broadcast_to(row_value, shape), 0.0), axis=1, keepdims=True)


def coefficients(stats, gain_row, shift_row, bias, channels, pixels):
    devices = stats.shape[0]
    count = pixels * (channels // GROUPS)
    mean_row = jnp.sum(stats, axis=0, keepdims=True) * (1.0 / devices)
    apart = jnp.sum(jnp.square(stats - mean_row), axis=0, keepdims=True) * (1.0 / devices)
    shape = (channels, LANES)
    group = group_index(channels, shape)
    lane = lane_index(shape)

    def pick(row_value, first):
        return jnp.sum(jnp.where(lane == group + first, jnp.broadcast_to(row_value, shape), 0.0), axis=1, keepdims=True)

    mean = pick(mean_row, 0)
    spread = pick(mean_row, GROUPS) * (1.0 / count) + pick(apart, 0)
    slope = lax.rsqrt(spread + EPSILON) * column_of(gain_row, channels)
    offset = column_of(shift_row, channels) - mean * slope
    if bias is not None:
        offset = offset + column_of(bias[0][...], channels, bias[1]) * slope
    return jnp.broadcast_to(slope * 0.5, shape), jnp.broadcast_to(offset * 0.5, shape)


def activate(value, coef):
    half = value.astype(F32) * coef[0] + coef[1]
    return (half + half * jnp.tanh(half)).astype(BF16)


def group_stats(sums, squares, bias, channels, pixels, width):
    shape = (channels, LANES)
    lane = lane_index(shape)
    group = group_index(channels, shape)
    inside = lane < width
    mean = jnp.sum(jnp.where(inside, sums, 0.0), axis=1, keepdims=True) * (1.0 / pixels)
    second = jnp.sum(jnp.where(inside, squares, 0.0), axis=1, keepdims=True)
    spread = jnp.maximum(second - pixels * jnp.square(mean), 0.0)
    if bias is not None:
        mean = mean + column_of(bias[0][...], channels, bias[1])
    group_size = channels // GROUPS
    mean_row = jnp.sum(jnp.where(lane == group, mean, 0.0), axis=0, keepdims=True) * (1.0 / group_size)
    group_mean = jnp.sum(jnp.where(lane == group, mean_row, 0.0), axis=1, keepdims=True)
    total = spread + pixels * jnp.square(mean - group_mean)
    return mean_row + jnp.sum(jnp.where(lane == group + GROUPS, total, 0.0), axis=0, keepdims=True)


def frame_rows(taps, first, channels, width, block_rows, rows_of, upper, lower, west, east, place):
    stride = taps.shape[1] // 3
    together = min(block_rows, TOGETHER)
    lane = lane_index((channels, LANES))
    base = place * block_rows

    def put(row, value, hw, he):
        taps[row, pl.ds(first, channels)] = jnp.where(lane == 0, hw, turn(value, 1))
        taps[row, pl.ds(stride + first, channels)] = value
        taps[row, pl.ds(2 * stride + first, channels)] = jnp.where(lane == width - 1, he, turn(value, LANES - 1))

    def sides(row):
        return turn(west, (LANES - base - row) % LANES), turn(east, (2 * LANES + width - 1 - base - row) % LANES)

    zero = jnp.zeros((channels, LANES), BF16)
    hw, he = sides(-1)
    put(0, upper, jnp.where(place == 0, zero, hw), jnp.where(place == 0, zero, he))

    def body(step, carry):
        for k in range(together):
            row = step * together + k
            put(row + 1, rows_of(row), *sides(row))
        return carry

    lax.fori_loop(0, block_rows // together, body, 0)
    hw, he = sides(block_rows)
    put(block_rows + 1, lower, jnp.where(place == 1, zero, hw), jnp.where(place == 1, zero, he))


def convolve_rows(taps, weight_ref, raw_ref, block_rows):
    outputs = weight_ref.shape[0]
    together = min(block_rows, TOGETHER)
    depth = taps.shape[1] * 3
    weight = weight_ref[...]
    zero = jnp.zeros((outputs, LANES), F32)

    def body(step, carry):
        sums, squares = carry
        row = step * together
        for k in range(0, together, 2):
            window = jnp.concatenate(
                [taps[pl.ds(row + k + j, 3)].reshape(depth, LANES) for j in range(2)], axis=1
            )
            both = jnp.dot(weight, window, preferred_element_type=F32)
            for j in range(2):
                value = both[:, j * LANES : (j + 1) * LANES]
                raw_ref[row + k + j] = value.astype(raw_ref.dtype)
                sums = sums + value
                squares = squares + value * value
        return sums, squares

    return lax.fori_loop(0, block_rows // together, body, (zero, zero))


def pack_edges(raw_ref, pack_ref, block_rows, channels, width, depth, place):
    size = depth * channels
    together = min(block_rows, TOGETHER)
    lane = lane_index((channels, LANES))
    last = block_rows - 1
    for d in range(depth):
        outer = jnp.where(place == 0, d, last - d)
        pack_ref[pl.ds(d * channels, channels)] = raw_ref[outer].astype(BF16)
        pack_ref[pl.ds(size + d * channels, channels)] = raw_ref[last - outer].astype(BF16)

    spacing = 2 if width == LANES else 1

    def body(step, carry):
        carry = list(carry)
        for k in range(together):
            row = step * together + k
            value = raw_ref[row].astype(BF16)
            for d in range(depth):
                amount = spacing * row
                west = (lane == amount)
                east = lane == (amount + width - 1) % LANES
                if d:
                    left = turn(value, (amount + LANES - d) % LANES)
                    right = turn(value, (amount + d) % LANES)
                    carry[d] = jnp.where(west, left, jnp.where(east, right, carry[d]))
                else:
                    carry[d] = jnp.where(west | east, turn(value, amount), carry[d])
        return tuple(carry)

    zero = jnp.zeros((channels, LANES), BF16)
    columns = lax.fori_loop(0, block_rows // together, body, (zero,) * depth)
    for d in range(depth):
        pack_ref[pl.ds(2 * size + d * channels, channels)] = columns[d]


def send_stats(stat, held, stat_ref, sent):
    held[...] = jnp.broadcast_to(stat, held.shape)
    leave = pltpu.make_async_copy(held, stat_ref, sent)
    leave.start()
    return leave


def finish(taps, weight_ref, raw_ref, pack_ref, stat_ref, held, sent, bias, block_rows, channels, width, depth, place):
    sums, squares = convolve_rows(taps, weight_ref, raw_ref, block_rows)
    stat = group_stats(sums, squares, bias, channels, float(block_rows * width), width)
    leave = send_stats(stat, held, stat_ref, sent)
    if pack_ref is not None:
        pack_edges(raw_ref, pack_ref, block_rows, channels, width, depth, place)
    leave.wait()


WHOLE = pl.BlockSpec(memory_space=pltpu.VMEM)
SCALARS = pl.BlockSpec(memory_space=pltpu.SMEM)
ANYWHERE = pl.BlockSpec(memory_space=pl.ANY)
STATS = (pltpu.VMEM((DEVICES, LANES), F32), pltpu.SemaphoreType.DMA)


def call(body, operands, outs, scratch=(), limit=12):
    return pl.pallas_call(
        body,
        in_specs=[SCALARS] + [WHOLE] * (len(operands) - 1),
        out_specs=[ANYWHERE if s == (DEVICES, LANES) else WHOLE for s, _ in outs],
        out_shape=[jax.ShapeDtypeStruct(s, d) for s, d in outs],
        scratch_shapes=list(scratch),
        compiler_params=pltpu.CompilerParams(vmem_limit_bytes=limit * 1024 * 1024),
    )(*operands)


def edges_of_image(here, image):
    block_rows, channels, width = image.shape

    def body(here_ref, image_ref, pack_ref):
        pack_edges(image_ref, pack_ref, block_rows, channels, width, 1, here_ref[1])

    return call(body, (here, image), [((3 * channels, LANES), BF16)])[0]


def setup(here, seam_codes):
    count = seam_codes.shape[1]

    def body(here_ref, codes, scalar_ref):
        tile, place = here_ref[0], here_ref[1]

        def facing(steps, side):
            k = (side + 2 + codes[side, (tile + count + steps) % count]) % 4
            return k, jnp.where((k < 2) == (side < 2), 1, 0)

        odd = tile % 2 == 1
        north, south = facing(ROW_TILES, 0), facing(-ROW_TILES, 2)
        east, west = facing(-1, 1), facing(1, 3)
        scalar_ref[0] = place
        for k in range(2):
            scalar_ref[1 + k] = jnp.where(place == 0, north[k], south[k])
            scalar_ref[3 + k] = jnp.where(odd, east[k], west[k])
            scalar_ref[5 + k] = jnp.where(odd, west[k], east[k])
        scalar_ref[7] = jnp.where(odd, 1, 0)

    return pl.pallas_call(
        body,
        in_specs=[SCALARS, SCALARS],
        out_specs=SCALARS,
        out_shape=jax.ShapeDtypeStruct((8,), jnp.int32),
        compiler_params=pltpu.CompilerParams(vmem_limit_bytes=2 * 1024 * 1024),
    )(here, seam_codes)


def one_table(scalars, tables):
    def body(sc, *rest):
        table_refs, param_ref = rest[: len(tables)], rest[len(tables)]
        for k, table_ref in enumerate(table_refs):
            lines, columns = table_ref.shape
            param_ref[4 * k : 4 * k + lines, 0:columns] = table_ref[...]

    return call(body, (scalars, *tables), [((4 * len(tables), LANES), F32)])[0]


def strips(scalars, pack, partner, width):
    size = pack.shape[0] // 3
    half = width // 2

    def body(sc, mine_ref, their_ref, ns_ref, near_ref, far_ref):
        place = sc[0]

        def ordered(first):
            mine, theirs = mine_ref[pl.ds(first, size)], their_ref[pl.ds(first, size)]
            return [jnp.where(place == 0, mine, theirs), jnp.where(place == 0, theirs, mine)]

        sources = jnp.concatenate(ordered(0) + ordered(2 * size), axis=1)
        shape = (4 * LANES, LANES)
        row, column = lax.broadcasted_iota(jnp.int32, shape, 0), lane_index((1, LANES))
        spacing = 2 if width == LANES else 1
        for k, out in enumerate((ns_ref, near_ref, far_ref)):
            side = sc[1 + 2 * k]
            pixel = jnp.where(sc[2 + 2 * k] == 1, width - 1 - column, column)
            along_row = pixel + jnp.where(side == 0, 0, LANES)
            under = pixel >= half
            start = jnp.where(side == 1, width - 1, 0)
            lane = (start + spacing * jnp.where(under, pixel - half, pixel)) & (LANES - 1)
            along_column = lane + jnp.where(under, 3 * LANES, 2 * LANES)
            source = jnp.where((side == 0) | (side == 2), along_row, along_column)
            source = jnp.where(column < width, source, -1)
            pick = jnp.where(row == jnp.broadcast_to(source, shape), 1.0, 0.0).astype(BF16)
            out[...] = jnp.dot(sources, pick, preferred_element_type=F32).astype(BF16)

    outs = [((size, LANES), BF16)] * 3
    return call(body, (scalars, pack, partner), outs)


def norm_lines(param_ref, line):
    return param_ref[line : line + 1], param_ref[line + 4 : line + 5]


def west_east(scalars, near_ref, far_ref):
    near, far = near_ref[...], far_ref[...]
    odd = scalars[7] == 1
    return jnp.where(odd, near, far), jnp.where(odd, far, near)


def above_below(place, facing, inner):
    return jnp.where(place == 0, facing, inner), jnp.where(place == 0, inner, facing)


def first_stage(scalars, image, partner, ns, near, far, weight, bias):
    block_rows, channels, width = image.shape
    outputs = weight.shape[0]

    def body(sc, image_ref, partner_ref, ns_ref, near_ref, far_ref, weight_ref, bias_ref, *rest):
        raw_ref, pack_ref, stat_ref, taps, held, sent = rest
        place = sc[0]
        upper, lower = above_below(place, ns_ref[...], partner_ref[pl.ds(channels, channels)])
        west, east = west_east(sc, near_ref, far_ref)
        frame_rows(taps, 0, channels, width, block_rows, lambda r: image_ref[r], upper, lower, west, east, place)
        finish(taps, weight_ref, raw_ref, pack_ref, stat_ref, held, sent, (bias_ref, 0), block_rows, outputs, width, 1, place)

    return call(
        body,
        (scalars, image, partner, ns, near, far, weight, bias),
        [
            ((block_rows, outputs, LANES), BF16),
            ((3 * outputs, LANES), BF16),
            ((DEVICES, LANES), F32),
        ],
        [pltpu.VMEM((block_rows + 2, 3 * channels, LANES), BF16), *STATS],
    )


def plain_stage(scalars, raw, stats, partner, ns, near, far, weight, params, line, bias, first, width, depth):
    block_rows, channels, _ = raw.shape
    outputs = weight.shape[0]
    biased = bias is not None

    def body(sc, raw_in, stats_ref, partner_ref, ns_ref, near_ref, far_ref, weight_ref, param_ref, *rest):
        bias_row = None
        if biased:
            bias_row, rest = (rest[0], first), rest[1:]
        if depth:
            raw_ref, stat_ref, pack_ref, taps, held, sent = rest
        else:
            raw_ref, stat_ref, taps, held, sent = rest
            pack_ref = None
        place = sc[0]
        coef = coefficients(
            stats_ref[...], *norm_lines(param_ref, line), bias_row, channels, float(block_rows * width)
        )
        lane = lane_index((channels, LANES))
        clear = jnp.zeros((channels, LANES), BF16)

        def strip(value):
            return jnp.where(lane < width, activate(value, coef), clear)

        west, east = west_east(sc, near_ref, far_ref)
        upper, lower = above_below(place, strip(ns_ref[...]), activate(partner_ref[pl.ds(channels, channels)], coef))
        frame_rows(
            taps,
            0,
            channels,
            width,
            block_rows,
            lambda r: activate(raw_in[r], coef),
            upper,
            lower,
            strip(west),
            strip(east),
            place,
        )
        finish(
            taps, weight_ref, raw_ref, pack_ref, stat_ref, held, sent, None, block_rows, outputs, width, depth, place
        )

    outs = [((block_rows, outputs, LANES), BF16), ((DEVICES, LANES), F32)]
    if depth:
        outs.append(((3 * depth * outputs, LANES), BF16))
    operands = (scalars, raw, stats, partner, ns, near, far, weight, params)
    if biased:
        operands += (bias,)
    return call(body, operands, outs, [pltpu.VMEM((block_rows + 2, 3 * channels, LANES), BF16), *STATS])


def pool_stage(scalars, raw, stats, partner, ns, near, far, weight, params, bias):
    block_rows, channels, width = raw.shape
    low_rows, low_width = block_rows // 2, width // 2
    outputs = weight.shape[0]

    def body(
        sc, raw_in, stats_ref, partner_ref, ns_ref, near_ref, far_ref, weight_ref, param_ref, bias_ref,
        skip_ref, side_ref, raw_ref, pack_ref, stat_ref, taps, pooled, held, sent,
    ):
        place = sc[0]
        coef = coefficients(stats_ref[...], *norm_lines(param_ref, 1), None, channels, float(block_rows * width))
        shape = (2 * LANES, LANES)
        row, column = lax.broadcasted_iota(jnp.int32, shape, 0), lane_index(shape)
        gather = jnp.where(((row & (LANES - 1)) >> 1) == column, 0.25, 0.0).astype(BF16)

        def pool(outer, second):
            both = jnp.concatenate([outer, second], axis=1)
            return jnp.dot(both, gather, preferred_element_type=F32).astype(BF16)

        def lines(value):
            return activate(value[:channels], coef), activate(value[channels:], coef)

        west, east = west_east(sc, near_ref, far_ref)
        ns_lines, east_lines, west_lines = lines(ns_ref[...]), lines(east), lines(west)
        inner_lines = lines(partner_ref[pl.ds(2 * channels, 2 * channels)])
        upper, lower = above_below(place, ns_lines[0], inner_lines[0])
        side_ref[0] = upper
        side_ref[1] = lower
        side_ref[2] = west_lines[0]
        side_ref[3] = east_lines[0]

        def make(step, carry):
            for k in range(low_rows):
                row = step * low_rows + k
                first = activate(raw_in[2 * row], coef)
                second = activate(raw_in[2 * row + 1], coef)
                skip_ref[2 * row] = first
                skip_ref[2 * row + 1] = second
                pooled[row] = pool(first, second)
            return carry

        lax.fori_loop(0, 1, make, 0)
        upper, lower = above_below(place, pool(*ns_lines), pool(*inner_lines))
        frame_rows(
            taps,
            0,
            channels,
            low_width,
            low_rows,
            lambda r: pooled[r],
            upper,
            lower,
            pool(*west_lines),
            pool(*east_lines),
            place,
        )
        finish(taps, weight_ref, raw_ref, pack_ref, stat_ref, held, sent, (bias_ref, channels), low_rows, outputs, low_width, 1, place)

    return call(
        body,
        (scalars, raw, stats, partner, ns, near, far, weight, params, bias),
        [
            ((block_rows, channels, LANES), BF16),
            ((4, channels, LANES), BF16),
            ((low_rows, outputs, LANES), BF16),
            ((3 * outputs, LANES), BF16),
            ((DEVICES, LANES), F32),
        ],
        [
            pltpu.VMEM((low_rows + 2, 3 * channels, LANES), BF16),
            pltpu.VMEM((low_rows, channels, LANES), BF16),
            *STATS,
        ],
    )


def skip_stage(scalars, skip, sides, weight):
    block_rows, channels, width = skip.shape
    outputs = weight.shape[0]

    def body(sc, skip_ref, side_ref, weight_ref, part_ref, taps):
        frame_rows(
            taps,
            0,
            channels,
            width,
            block_rows,
            lambda r: skip_ref[r],
            side_ref[0],
            side_ref[1],
            side_ref[2],
            side_ref[3],
            sc[0],
        )
        convolve_rows(taps, weight_ref, part_ref, block_rows)

    return call(
        body,
        (scalars, skip, sides, weight),
        [((block_rows, outputs, LANES), BF16)],
        [pltpu.VMEM((block_rows + 2, 3 * channels, LANES), BF16)],
    )[0]


def decode_stage(scalars, raw, stats, partner, ns, near, far, part, deep_weight, params):
    low_rows, channels, _ = raw.shape
    block_rows, outputs, width = part.shape
    low_width = width // 2

    def body(
        sc, raw_in, stats_ref, partner_ref, ns_ref, near_ref, far_ref, part_ref, deep_ref, param_ref,
        raw_ref, pack_ref, stat_ref, deep_taps, wide, held, sent,
    ):
        place = sc[0]
        coef = coefficients(
            stats_ref[...], *norm_lines(param_ref, 9), None, channels, float(low_rows * low_width)
        )
        shape = (LANES, LANES)
        row, column = lax.broadcasted_iota(jnp.int32, shape, 0), lane_index(shape)
        spread = jnp.where(row == column >> 1, 1.0, 0.0).astype(BF16)

        lane = lane_index((channels, LANES))

        def kept(value):
            return jnp.where(lane < low_width, activate(value, coef), jnp.zeros((channels, LANES), BF16))

        def widen(value):
            return jnp.dot(kept(value), spread, preferred_element_type=F32).astype(BF16)

        def make(step, carry):
            for k in range(low_rows):
                wide[step * low_rows + k] = widen(raw_in[step * low_rows + k])
            return carry

        lax.fori_loop(0, 1, make, 0)
        west, east = west_east(sc, near_ref, far_ref)
        upper, lower = above_below(place, widen(ns_ref[...]), widen(partner_ref[pl.ds(channels, channels)]))
        frame_rows(
            deep_taps, 0, channels, width, low_rows, lambda r: wide[r], upper, lower, kept(west), kept(east), place
        )
        deep_weights = deep_ref[...]
        zero = jnp.zeros((outputs, LANES), F32)
        together = 32

        def convolve(step, carry):
            sums, squares = carry
            for k in range(0, together, 2):
                low = step * together + k
                window = jnp.concatenate(
                    [deep_taps[pl.ds(low + j, 3)].reshape(9 * channels, LANES) for j in range(2)], axis=1
                )
                deep = jnp.dot(deep_weights, window, preferred_element_type=F32)
                for j in range(2):
                    high = 2 * (low + j)
                    for i in range(2):
                        value = part_ref[high + i].astype(F32)
                        value = value + deep[i * outputs : (i + 1) * outputs, j * LANES : (j + 1) * LANES]
                        raw_ref[high + i] = value.astype(BF16)
                        sums = sums + value
                        squares = squares + value * value
            return sums, squares

        sums, squares = lax.fori_loop(0, low_rows // together, convolve, (zero, zero))
        stat = group_stats(sums, squares, None, outputs, float(block_rows * width), width)
        leave = send_stats(stat, held, stat_ref, sent)
        pack_edges(raw_ref, pack_ref, block_rows, outputs, width, 1, place)
        leave.wait()

    return call(
        body,
        (scalars, raw, stats, partner, ns, near, far, part, deep_weight, params),
        [((block_rows, outputs, LANES), BF16), ((3 * outputs, LANES), BF16), ((DEVICES, LANES), F32)],
        [
            pltpu.VMEM((low_rows + 2, 3 * channels, LANES), BF16),
            pltpu.VMEM((low_rows, channels, LANES), BF16),
            *STATS,
        ],
    )


def project_stage(scalars, raw, stats, weight, params, kept):
    block_rows, channels, width = raw.shape

    def body(sc, raw_in, stats_ref, weight_ref, param_ref, out_ref):
        coef = coefficients(stats_ref[...], *norm_lines(param_ref, 3), None, channels, float(block_rows * width))
        project = weight_ref[...]

        def make(step, carry):
            for k in range(0, 64, 2):
                row = step * 64 + k
                both = jnp.concatenate([activate(raw_in[row], coef), activate(raw_in[row + 1], coef)], axis=1)
                result = jnp.dot(project, both, preferred_element_type=F32).astype(BF16)
                out_ref[row] = result[:kept, :LANES]
                out_ref[row + 1] = result[:kept, LANES:]
            return carry

        lax.fori_loop(0, block_rows // 64, make, 0)

    return call(body, (scalars, raw, stats, weight, params), [((block_rows, kept, LANES), BF16)])[0]


def vertical(value):
    count = lax.axis_size(TILE)
    pairs = []
    for t in range(count):
        pairs.append((2 * t, 2 * ((t + ROW_TILES) % count)))
        pairs.append((2 * t + 1, 2 * ((t - ROW_TILES) % count) + 1))
    return lax.ppermute(value, TILE_SPLIT, pairs)


def exchange(scalars, pack, width, later=()):
    partner = lax.ppermute(pack, "split", [(0, 1), (1, 0)])
    ns, near, far = strips(scalars, pack, partner, width)
    (ns, near, far), later = lax.optimization_barrier(((ns, near, far), later)) if later else ((ns, near, far), later)
    count = lax.axis_size(TILE)
    far = lax.ppermute(far, TILE, [(t, (t - 1 + 2 * (t % 2)) % count) for t in range(count)])
    near = lax.ppermute(near, TILE, [(t, t + 1 - 2 * (t % 2)) for t in range(count)])
    ns = vertical(ns)
    return (partner, ns, near, far), later


def share(stat):
    copies = stat.reshape(DEVICES, 1, LANES)
    return lax.all_to_all(copies, TILE_SPLIT, 0, 0).reshape(DEVICES, LANES)


def meet(scalars, pack, stat, width):
    received = exchange(scalars, pack, width)[0] if pack is not None else None
    return (share(stat) if stat is not None else None), received


def embedding(timestep, time_weight, bias_upper, bias_lower):
    moment = timestep[0].astype(F32)
    half_width = time_weight.shape[0] // 2
    frequencies = jnp.exp(-math.log(10000.0) * jnp.arange(half_width, dtype=F32) / half_width)
    angles = moment * frequencies
    features = jnp.concatenate([jnp.sin(angles), jnp.cos(angles)])[None, :]
    embedded = jax.nn.silu(jnp.dot(features, time_weight, precision=lax.Precision.HIGHEST))
    both = jnp.concatenate([bias_upper, bias_lower], axis=1)
    biases = jnp.dot(embedded, both, precision=lax.Precision.HIGHEST)
    return biases


def flat_kernel(kernel):
    return jnp.transpose(kernel, (2, 0, 1, 3)).reshape(kernel.shape[2], -1)


def deep_kernel(kernel):
    wide = kernel.astype(F32)
    none = jnp.zeros_like(wide[0])
    even = jnp.stack([wide[0], wide[1] + wide[2], none])
    odd = jnp.stack([none, wide[0] + wide[1], wide[2]])
    both = jnp.stack([even, odd]).astype(BF16)
    return jnp.transpose(both, (0, 3, 1, 2, 4)).reshape(2 * kernel.shape[2], -1)


def per_device(
    noisy_image,
    seam_codes,
    timestep,
    time_weight,
    bias_upper,
    bias_lower,
    kernel_upper_first,
    kernel_upper_second,
    kernel_lower_first,
    kernel_lower_second,
    kernel_decode_first,
    kernel_decode_second,
    output_weight,
    gains_upper,
    shifts_upper,
    gains_lower,
    shifts_lower,
):
    here = jnp.stack([lax.axis_index(TILE), lax.axis_index("split")]).astype(jnp.int32)
    channels, _, width = noisy_image.shape[1:]
    padding = kernel_upper_first.shape[2] - channels
    image = jnp.transpose(jnp.pad(noisy_image[0], ((0, padding), (0, 0), (0, 0))), (1, 0, 2))
    low_width = width // 2
    width_one = kernel_upper_first.shape[2]

    pack = edges_of_image(here, image)
    scalars = setup(here, seam_codes.T)
    early = (timestep, time_weight, bias_upper, bias_lower, kernel_upper_first, kernel_upper_second)
    late = (kernel_lower_first, kernel_lower_second, kernel_decode_first, kernel_decode_second, output_weight)
    received, early = exchange(scalars, pack, width, early)
    params = one_table(scalars, (gains_upper, shifts_upper, gains_lower, shifts_lower))
    timestep, time_weight, bias_upper, bias_lower, kernel_upper_first, kernel_upper_second = early
    biases = embedding(timestep, time_weight, bias_upper, bias_lower)
    weights = (
        flat_kernel(jnp.pad(kernel_upper_first, ((0, 0), (0, 0), (0, 0), (0, padding)))),
        flat_kernel(kernel_upper_second),
        biases,
    )
    received, (upper_first, upper_second, biases) = lax.optimization_barrier((received, weights))
    raw, pack, stat = first_stage(scalars, image, *received, upper_first, biases)

    received, late = exchange(scalars, pack, width, late)
    stats = share(stat)
    kernel_lower_first, kernel_lower_second, kernel_decode_first, kernel_decode_second, output_weight = late
    weights = (
        flat_kernel(kernel_lower_first),
        flat_kernel(kernel_lower_second),
        flat_kernel(kernel_decode_first[..., -width_one:]),
        deep_kernel(kernel_decode_first[..., :-width_one]),
        flat_kernel(kernel_decode_second),
        jnp.pad(output_weight, ((0, padding), (0, 0))),
    )
    received, weights = lax.optimization_barrier((received, weights))
    lower_first, lower_second, decode_skip, decode_deep, decode_second, project = weights
    raw, stat, pack = plain_stage(
        scalars, raw, stats, *received, upper_second, params, 0, biases, 0, width, 2
    )

    stats, received = meet(scalars, pack, stat, width)
    skip, sides, raw, pack, stat = pool_stage(
        scalars, raw, stats, *received, lower_first, params, biases
    )

    stats, received = meet(scalars, pack, stat, low_width)
    part = skip_stage(scalars, skip, sides, decode_skip)
    raw, stat, pack = plain_stage(
        scalars, raw, stats, *received, lower_second, params, 8, biases, width_one,
        low_width, 1,
    )

    stats, received = meet(scalars, pack, stat, low_width)
    raw, pack, stat = decode_stage(
        scalars, raw, stats, *received, part, decode_deep, params
    )

    stats, received = meet(scalars, pack, stat, width)
    raw, stat = plain_stage(
        scalars, raw, stats, *received, decode_second, params, 2, None, 0, width, 0
    )

    stats, _ = meet(scalars, None, stat, width)
    result = project_stage(scalars, raw, stats, project, params, channels)
    return jnp.transpose(result, (1, 0, 2))[None]


def solution(mesh):
    torus = Mesh(
        mesh.devices.reshape(4, 4, 2, 2, mesh.shape["split"]),
        ("tile_0", "tile_1", "tile_2", "tile_3", "split"),
    )
    return jax.shard_map(
        per_device,
        mesh=torus,
        in_specs=(P(TILE, None, "split", None),) + (P(),) * 16,
        out_specs=P(TILE, None, "split", None),
        check_vma=False,
    )
```

```python
import math

import jax
import jax.numpy as jnp
from jax import lax
from jax.experimental import pallas as pl
from jax.experimental.pallas import tpu as pltpu
from jax.sharding import Mesh
from jax.sharding import PartitionSpec as P


GROUPS = 8
ROW_TILES = 4
TILE = ("tile_0", "tile_1", "tile_2", "tile_3")
TILE_SPLIT = ("tile_0", "tile_1", "tile_2", "tile_3", "split")
EPSILON = 1e-05
LANES = 128
DEVICES = 128
TOGETHER = 64
F32 = jnp.float32
BF16 = jnp.bfloat16


def lane_index(shape):
    return lax.broadcasted_iota(jnp.int32, shape, 1)


def turn(value, amount):
    return pltpu.roll(value, amount, 1)


def group_index(channels, shape):
    row = lax.broadcasted_iota(jnp.int32, shape, 0)
    return (row * 43) >> (8 if channels == 48 else 9)


def column_of(row_value, channels, first=0):
    shape = (channels, row_value.shape[1])
    on_diagonal = lax.broadcasted_iota(jnp.int32, shape, 0) + first == lane_index(shape)
    return jnp.sum(jnp.where(on_diagonal, jnp.broadcast_to(row_value, shape), 0.0), axis=1, keepdims=True)


def coefficients(stats, gain_row, shift_row, bias, channels, pixels):
    devices = stats.shape[0]
    count = pixels * (channels // GROUPS)
    mean_row = jnp.sum(stats, axis=0, keepdims=True) * (1.0 / devices)
    apart = jnp.sum(jnp.square(stats - mean_row), axis=0, keepdims=True) * (1.0 / devices)
    shape = (channels, LANES)
    group = group_index(channels, shape)
    lane = lane_index(shape)

    def pick(row_value, first):
        return jnp.sum(jnp.where(lane == group + first, jnp.broadcast_to(row_value, shape), 0.0), axis=1, keepdims=True)

    mean = pick(mean_row, 0)
    spread = pick(mean_row, GROUPS) * (1.0 / count) + pick(apart, 0)
    slope = lax.rsqrt(spread + EPSILON) * column_of(gain_row, channels)
    offset = column_of(shift_row, channels) - mean * slope
    if bias is not None:
        offset = offset + column_of(bias[0][...], channels, bias[1]) * slope
    return jnp.broadcast_to(slope * 0.5, shape), jnp.broadcast_to(offset * 0.5, shape)


def activate(value, coef):
    half = value.astype(F32) * coef[0] + coef[1]
    return (half + half * jnp.tanh(half)).astype(BF16)


def group_stats(sums, squares, bias, channels, pixels, width):
    shape = (channels, LANES)
    lane = lane_index(shape)
    group = group_index(channels, shape)
    inside = lane < width
    mean = jnp.sum(jnp.where(inside, sums, 0.0), axis=1, keepdims=True) * (1.0 / pixels)
    second = jnp.sum(jnp.where(inside, squares, 0.0), axis=1, keepdims=True)
    spread = jnp.maximum(second - pixels * jnp.square(mean), 0.0)
    if bias is not None:
        mean = mean + column_of(bias[0][...], channels, bias[1])
    group_size = channels // GROUPS
    mean_row = jnp.sum(jnp.where(lane == group, mean, 0.0), axis=0, keepdims=True) * (1.0 / group_size)
    group_mean = jnp.sum(jnp.where(lane == group, mean_row, 0.0), axis=1, keepdims=True)
    total = spread + pixels * jnp.square(mean - group_mean)
    return mean_row + jnp.sum(jnp.where(lane == group + GROUPS, total, 0.0), axis=0, keepdims=True)


def frame_rows(taps, first, channels, width, block_rows, rows_of, upper, lower, west, east, place):
    stride = taps.shape[1] // 3
    together = min(block_rows, TOGETHER)
    lane = lane_index((channels, LANES))
    base = place * block_rows

    def put(row, value, hw, he):
        taps[row, pl.ds(first, channels)] = jnp.where(lane == 0, hw, turn(value, 1))
        taps[row, pl.ds(stride + first, channels)] = value
        taps[row, pl.ds(2 * stride + first, channels)] = jnp.where(lane == width - 1, he, turn(value, LANES - 1))

    def sides(row):
        return turn(west, (LANES - base - row) % LANES), turn(east, (2 * LANES + width - 1 - base - row) % LANES)

    zero = jnp.zeros((channels, LANES), BF16)
    hw, he = sides(-1)
    put(0, upper, jnp.where(place == 0, zero, hw), jnp.where(place == 0, zero, he))

    def body(step, carry):
        for k in range(together):
            row = step * together + k
            put(row + 1, rows_of(row), *sides(row))
        return carry

    lax.fori_loop(0, block_rows // together, body, 0)
    hw, he = sides(block_rows)
    put(block_rows + 1, lower, jnp.where(place == 1, zero, hw), jnp.where(place == 1, zero, he))


def convolve_rows(taps, weight_ref, raw_ref, block_rows):
    outputs = weight_ref.shape[0]
    together = min(block_rows, TOGETHER)
    depth = taps.shape[1] * 3
    weight = weight_ref[...]
    zero = jnp.zeros((outputs, LANES), F32)

    def body(step, carry):
        sums, squares = carry
        row = step * together
        for k in range(0, together, 2):
            window = jnp.concatenate(
                [taps[pl.ds(row + k + j, 3)].reshape(depth, LANES) for j in range(2)], axis=1
            )
            both = jnp.dot(weight, window, preferred_element_type=F32)
            for j in range(2):
                value = both[:, j * LANES : (j + 1) * LANES]
                raw_ref[row + k + j] = value.astype(raw_ref.dtype)
                sums = sums + value
                squares = squares + value * value
        return sums, squares

    return lax.fori_loop(0, block_rows // together, body, (zero, zero))


def pack_edges(raw_ref, pack_ref, block_rows, channels, width, depth, place):
    size = depth * channels
    together = min(block_rows, TOGETHER)
    lane = lane_index((channels, LANES))
    last = block_rows - 1
    for d in range(depth):
        outer = jnp.where(place == 0, d, last - d)
        pack_ref[pl.ds(d * channels, channels)] = raw_ref[outer].astype(BF16)
        pack_ref[pl.ds(size + d * channels, channels)] = raw_ref[last - outer].astype(BF16)

    spacing = 2 if width == LANES else 1

    def body(step, carry):
        carry = list(carry)
        for k in range(together):
            row = step * together + k
            value = raw_ref[row].astype(BF16)
            for d in range(depth):
                amount = spacing * row
                west = (lane == amount)
                east = lane == (amount + width - 1) % LANES
                if d:
                    left = turn(value, (amount + LANES - d) % LANES)
                    right = turn(value, (amount + d) % LANES)
                    carry[d] = jnp.where(west, left, jnp.where(east, right, carry[d]))
                else:
                    carry[d] = jnp.where(west | east, turn(value, amount), carry[d])
        return tuple(carry)

    zero = jnp.zeros((channels, LANES), BF16)
    columns = lax.fori_loop(0, block_rows // together, body, (zero,) * depth)
    for d in range(depth):
        pack_ref[pl.ds(2 * size + d * channels, channels)] = columns[d]


def send_stats(stat, held, stat_ref, sent):
    held[...] = jnp.broadcast_to(stat, held.shape)
    leave = pltpu.make_async_copy(held, stat_ref, sent)
    leave.start()
    return leave


def finish(taps, weight_ref, raw_ref, pack_ref, stat_ref, held, sent, bias, block_rows, channels, width, depth, place):
    sums, squares = convolve_rows(taps, weight_ref, raw_ref, block_rows)
    stat = group_stats(sums, squares, bias, channels, float(block_rows * width), width)
    leave = send_stats(stat, held, stat_ref, sent)
    if pack_ref is not None:
        pack_edges(raw_ref, pack_ref, block_rows, channels, width, depth, place)
    leave.wait()


WHOLE = pl.BlockSpec(memory_space=pltpu.VMEM)
SCALARS = pl.BlockSpec(memory_space=pltpu.SMEM)
ANYWHERE = pl.BlockSpec(memory_space=pl.ANY)
STATS = (pltpu.VMEM((DEVICES, LANES), F32), pltpu.SemaphoreType.DMA)


def call(body, operands, outs, scratch=(), limit=12):
    return pl.pallas_call(
        body,
        in_specs=[SCALARS] + [WHOLE] * (len(operands) - 1),
        out_specs=[ANYWHERE if s == (DEVICES, LANES) else WHOLE for s, _ in outs],
        out_shape=[jax.ShapeDtypeStruct(s, d) for s, d in outs],
        scratch_shapes=list(scratch),
        compiler_params=pltpu.CompilerParams(vmem_limit_bytes=limit * 1024 * 1024),
    )(*operands)


def edges_of_image(here, image):
    block_rows, channels, width = image.shape

    def body(here_ref, image_ref, pack_ref):
        pack_edges(image_ref, pack_ref, block_rows, channels, width, 1, here_ref[1])

    return call(body, (here, image), [((3 * channels, LANES), BF16)])[0]


def setup(here, seam_codes):
    count = seam_codes.shape[1]

    def body(here_ref, codes, scalar_ref):
        tile, place = here_ref[0], here_ref[1]

        def facing(steps, side):
            k = (side + 2 + codes[side, (tile + count + steps) % count]) % 4
            return k, jnp.where((k < 2) == (side < 2), 1, 0)

        odd = tile % 2 == 1
        north, south = facing(ROW_TILES, 0), facing(-ROW_TILES, 2)
        east, west = facing(-1, 1), facing(1, 3)
        scalar_ref[0] = place
        for k in range(2):
            scalar_ref[1 + k] = jnp.where(place == 0, north[k], south[k])
            scalar_ref[3 + k] = jnp.where(odd, east[k], west[k])
            scalar_ref[5 + k] = jnp.where(odd, west[k], east[k])
        scalar_ref[7] = jnp.where(odd, 1, 0)

    return pl.pallas_call(
        body,
        in_specs=[SCALARS, SCALARS],
        out_specs=SCALARS,
        out_shape=jax.ShapeDtypeStruct((8,), jnp.int32),
        compiler_params=pltpu.CompilerParams(vmem_limit_bytes=2 * 1024 * 1024),
    )(here, seam_codes)


def one_table(scalars, tables):
    def body(sc, *rest):
        table_refs, param_ref = rest[: len(tables)], rest[len(tables)]
        for k, table_ref in enumerate(table_refs):
            lines, columns = table_ref.shape
            param_ref[4 * k : 4 * k + lines, 0:columns] = table_ref[...]

    return call(body, (scalars, *tables), [((4 * len(tables), LANES), F32)])[0]


def strips(scalars, pack, partner, width):
    size = pack.shape[0] // 3
    half = width // 2

    def body(sc, mine_ref, their_ref, ns_ref, near_ref, far_ref):
        place = sc[0]

        def ordered(first):
            mine, theirs = mine_ref[pl.ds(first, size)], their_ref[pl.ds(first, size)]
            return [jnp.where(place == 0, mine, theirs), jnp.where(place == 0, theirs, mine)]

        sources = jnp.concatenate(ordered(0) + ordered(2 * size), axis=1)
        shape = (4 * LANES, LANES)
        row, column = lax.broadcasted_iota(jnp.int32, shape, 0), lane_index((1, LANES))
        spacing = 2 if width == LANES else 1
        for k, out in enumerate((ns_ref, near_ref, far_ref)):
            side = sc[1 + 2 * k]
            pixel = jnp.where(sc[2 + 2 * k] == 1, width - 1 - column, column)
            along_row = pixel + jnp.where(side == 0, 0, LANES)
            under = pixel >= half
            start = jnp.where(side == 1, width - 1, 0)
            lane = (start + spacing * jnp.where(under, pixel - half, pixel)) & (LANES - 1)
            along_column = lane + jnp.where(under, 3 * LANES, 2 * LANES)
            source = jnp.where((side == 0) | (side == 2), along_row, along_column)
            source = jnp.where(column < width, source, -1)
            pick = jnp.where(row == jnp.broadcast_to(source, shape), 1.0, 0.0).astype(BF16)
            out[...] = jnp.dot(sources, pick, preferred_element_type=F32).astype(BF16)

    outs = [((size, LANES), BF16)] * 3
    return call(body, (scalars, pack, partner), outs)


def norm_lines(param_ref, line):
    return param_ref[line : line + 1], param_ref[line + 4 : line + 5]


def west_east(scalars, near_ref, far_ref):
    near, far = near_ref[...], far_ref[...]
    odd = scalars[7] == 1
    return jnp.where(odd, near, far), jnp.where(odd, far, near)


def above_below(place, facing, inner):
    return jnp.where(place == 0, facing, inner), jnp.where(place == 0, inner, facing)


def coef_stage(scalars, stats, params, line, bias, first, channels, pixels):
    def body(sc, stats_ref, param_ref, *rest):
        bias_at = (rest[0], first) if bias is not None else None
        slope, offset = coefficients(stats_ref[...], *norm_lines(param_ref, line), bias_at, channels, float(pixels))
        rest[-1][0] = slope
        rest[-1][1] = offset

    operands = (scalars, stats, params) + ((bias,) if bias is not None else ())
    return call(body, operands, [((2, channels, LANES), F32)])[0]


def first_stage(scalars, image, partner, ns, near, far, weight, bias):
    block_rows, channels, width = image.shape
    outputs = weight.shape[0]

    def body(sc, image_ref, partner_ref, ns_ref, near_ref, far_ref, weight_ref, bias_ref, *rest):
        raw_ref, pack_ref, stat_ref, taps, held, sent = rest
        place = sc[0]
        upper, lower = above_below(place, ns_ref[...], partner_ref[pl.ds(channels, channels)])
        west, east = west_east(sc, near_ref, far_ref)
        frame_rows(taps, 0, channels, width, block_rows, lambda r: image_ref[r], upper, lower, west, east, place)
        finish(taps, weight_ref, raw_ref, pack_ref, stat_ref, held, sent, (bias_ref, 0), block_rows, outputs, width, 1, place)

    return call(
        body,
        (scalars, image, partner, ns, near, far, weight, bias),
        [
            ((block_rows, outputs, LANES), BF16),
            ((3 * outputs, LANES), BF16),
            ((DEVICES, LANES), F32),
        ],
        [pltpu.VMEM((block_rows + 2, 3 * channels, LANES), BF16), *STATS],
    )


def plain_stage(scalars, raw, stats, partner, ns, near, far, weight, params, bias, width, depth):
    block_rows, channels, _ = raw.shape
    outputs = weight.shape[0]
    biased = bias is not None

    def body(sc, raw_in, stats_ref, partner_ref, ns_ref, near_ref, far_ref, weight_ref, param_ref, *rest):
        if biased:
            rest = rest[1:]
        if depth:
            raw_ref, stat_ref, pack_ref, taps, held, sent = rest
        else:
            raw_ref, stat_ref, taps, held, sent = rest
            pack_ref = None
        place = sc[0]
        coef = (stats_ref[0], stats_ref[1])
        lane = lane_index((channels, LANES))
        clear = jnp.zeros((channels, LANES), BF16)

        def strip(value):
            return jnp.where(lane < width, activate(value, coef), clear)

        west, east = west_east(sc, near_ref, far_ref)
        upper, lower = above_below(place, strip(ns_ref[...]), activate(partner_ref[pl.ds(channels, channels)], coef))
        frame_rows(
            taps,
            0,
            channels,
            width,
            block_rows,
            lambda r: activate(raw_in[r], coef),
            upper,
            lower,
            strip(west),
            strip(east),
            place,
        )
        finish(
            taps, weight_ref, raw_ref, pack_ref, stat_ref, held, sent, None, block_rows, outputs, width, depth, place
        )

    outs = [((block_rows, outputs, LANES), BF16), ((DEVICES, LANES), F32)]
    if depth:
        outs.append(((3 * depth * outputs, LANES), BF16))
    operands = (scalars, raw, stats, partner, ns, near, far, weight, params)
    if biased:
        operands += (bias,)
    return call(body, operands, outs, [pltpu.VMEM((block_rows + 2, 3 * channels, LANES), BF16), *STATS])


def pool_stage(scalars, raw, stats, partner, ns, near, far, weight, params, bias):
    block_rows, channels, width = raw.shape
    low_rows, low_width = block_rows // 2, width // 2
    outputs = weight.shape[0]

    def body(
        sc, raw_in, stats_ref, partner_ref, ns_ref, near_ref, far_ref, weight_ref, param_ref, bias_ref,
        skip_ref, side_ref, raw_ref, pack_ref, stat_ref, taps, pooled, held, sent,
    ):
        place = sc[0]
        coef = (stats_ref[0], stats_ref[1])
        shape = (2 * LANES, LANES)
        row, column = lax.broadcasted_iota(jnp.int32, shape, 0), lane_index(shape)
        gather = jnp.where(((row & (LANES - 1)) >> 1) == column, 0.25, 0.0).astype(BF16)

        def pool(outer, second):
            both = jnp.concatenate([outer, second], axis=1)
            return jnp.dot(both, gather, preferred_element_type=F32).astype(BF16)

        def lines(value):
            return activate(value[:channels], coef), activate(value[channels:], coef)

        west, east = west_east(sc, near_ref, far_ref)
        ns_lines, east_lines, west_lines = lines(ns_ref[...]), lines(east), lines(west)
        inner_lines = lines(partner_ref[pl.ds(2 * channels, 2 * channels)])
        upper, lower = above_below(place, ns_lines[0], inner_lines[0])
        side_ref[0] = upper
        side_ref[1] = lower
        side_ref[2] = west_lines[0]
        side_ref[3] = east_lines[0]

        def make(step, carry):
            for k in range(low_rows):
                row = step * low_rows + k
                first = activate(raw_in[2 * row], coef)
                second = activate(raw_in[2 * row + 1], coef)
                skip_ref[2 * row] = first
                skip_ref[2 * row + 1] = second
                pooled[row] = pool(first, second)
            return carry

        lax.fori_loop(0, 1, make, 0)
        upper, lower = above_below(place, pool(*ns_lines), pool(*inner_lines))
        frame_rows(
            taps,
            0,
            channels,
            low_width,
            low_rows,
            lambda r: pooled[r],
            upper,
            lower,
            pool(*west_lines),
            pool(*east_lines),
            place,
        )
        finish(taps, weight_ref, raw_ref, pack_ref, stat_ref, held, sent, (bias_ref, channels), low_rows, outputs, low_width, 1, place)

    return call(
        body,
        (scalars, raw, stats, partner, ns, near, far, weight, params, bias),
        [
            ((block_rows, channels, LANES), BF16),
            ((4, channels, LANES), BF16),
            ((low_rows, outputs, LANES), BF16),
            ((3 * outputs, LANES), BF16),
            ((DEVICES, LANES), F32),
        ],
        [
            pltpu.VMEM((low_rows + 2, 3 * channels, LANES), BF16),
            pltpu.VMEM((low_rows, channels, LANES), BF16),
            *STATS,
        ],
    )


def skip_stage(scalars, skip, sides, weight):
    block_rows, channels, width = skip.shape
    outputs = weight.shape[0]

    def body(sc, skip_ref, side_ref, weight_ref, part_ref, taps):
        frame_rows(
            taps,
            0,
            channels,
            width,
            block_rows,
            lambda r: skip_ref[r],
            side_ref[0],
            side_ref[1],
            side_ref[2],
            side_ref[3],
            sc[0],
        )
        convolve_rows(taps, weight_ref, part_ref, block_rows)

    return call(
        body,
        (scalars, skip, sides, weight),
        [((block_rows, outputs, LANES), BF16)],
        [pltpu.VMEM((block_rows + 2, 3 * channels, LANES), BF16)],
    )[0]


def decode_stage(scalars, raw, stats, partner, ns, near, far, part, deep_weight, params):
    low_rows, channels, _ = raw.shape
    block_rows, outputs, width = part.shape
    low_width = width // 2

    def body(
        sc, raw_in, stats_ref, partner_ref, ns_ref, near_ref, far_ref, part_ref, deep_ref, param_ref,
        raw_ref, pack_ref, stat_ref, deep_taps, wide, held, sent,
    ):
        place = sc[0]
        coef = (stats_ref[0], stats_ref[1])
        shape = (LANES, LANES)
        row, column = lax.broadcasted_iota(jnp.int32, shape, 0), lane_index(shape)
        spread = jnp.where(row == column >> 1, 1.0, 0.0).astype(BF16)

        lane = lane_index((channels, LANES))

        def kept(value):
            return jnp.where(lane < low_width, activate(value, coef), jnp.zeros((channels, LANES), BF16))

        def widen(value):
            return jnp.dot(kept(value), spread, preferred_element_type=F32).astype(BF16)

        def make(step, carry):
            for k in range(low_rows):
                wide[step * low_rows + k] = widen(raw_in[step * low_rows + k])
            return carry

        lax.fori_loop(0, 1, make, 0)
        west, east = west_east(sc, near_ref, far_ref)
        upper, lower = above_below(place, widen(ns_ref[...]), widen(partner_ref[pl.ds(channels, channels)]))
        frame_rows(
            deep_taps, 0, channels, width, low_rows, lambda r: wide[r], upper, lower, kept(west), kept(east), place
        )
        deep_weights = deep_ref[...]
        zero = jnp.zeros((outputs, LANES), F32)
        together = 32

        def convolve(step, carry):
            sums, squares = carry
            for k in range(0, together, 2):
                low = step * together + k
                window = jnp.concatenate(
                    [deep_taps[pl.ds(low + j, 3)].reshape(9 * channels, LANES) for j in range(2)], axis=1
                )
                deep = jnp.dot(deep_weights, window, preferred_element_type=F32)
                for j in range(2):
                    high = 2 * (low + j)
                    for i in range(2):
                        value = part_ref[high + i].astype(F32)
                        value = value + deep[i * outputs : (i + 1) * outputs, j * LANES : (j + 1) * LANES]
                        raw_ref[high + i] = value.astype(BF16)
                        sums = sums + value
                        squares = squares + value * value
            return sums, squares

        sums, squares = lax.fori_loop(0, low_rows // together, convolve, (zero, zero))
        stat = group_stats(sums, squares, None, outputs, float(block_rows * width), width)
        leave = send_stats(stat, held, stat_ref, sent)
        pack_edges(raw_ref, pack_ref, block_rows, outputs, width, 1, place)
        leave.wait()

    return call(
        body,
        (scalars, raw, stats, partner, ns, near, far, part, deep_weight, params),
        [((block_rows, outputs, LANES), BF16), ((3 * outputs, LANES), BF16), ((DEVICES, LANES), F32)],
        [
            pltpu.VMEM((low_rows + 2, 3 * channels, LANES), BF16),
            pltpu.VMEM((low_rows, channels, LANES), BF16),
            *STATS,
        ],
    )


def project_stage(scalars, raw, stats, weight, params, kept):
    block_rows, channels, width = raw.shape

    def body(sc, raw_in, stats_ref, weight_ref, param_ref, out_ref):
        coef = coefficients(stats_ref[...], *norm_lines(param_ref, 3), None, channels, float(block_rows * width))
        project = weight_ref[...]

        def make(step, carry):
            for k in range(0, 64, 2):
                row = step * 64 + k
                both = jnp.concatenate([activate(raw_in[row], coef), activate(raw_in[row + 1], coef)], axis=1)
                result = jnp.dot(project, both, preferred_element_type=F32).astype(BF16)
                out_ref[row] = result[:kept, :LANES]
                out_ref[row + 1] = result[:kept, LANES:]
            return carry

        lax.fori_loop(0, block_rows // 64, make, 0)

    return call(body, (scalars, raw, stats, weight, params), [((block_rows, kept, LANES), BF16)])[0]


def vertical(value):
    count = lax.axis_size(TILE)
    pairs = []
    for t in range(count):
        pairs.append((2 * t, 2 * ((t + ROW_TILES) % count)))
        pairs.append((2 * t + 1, 2 * ((t - ROW_TILES) % count) + 1))
    return lax.ppermute(value, TILE_SPLIT, pairs)


def exchange(scalars, pack, width, later=()):
    partner = lax.ppermute(pack, "split", [(0, 1), (1, 0)])
    ns, near, far = strips(scalars, pack, partner, width)
    (ns, near, far), later = lax.optimization_barrier(((ns, near, far), later)) if later else ((ns, near, far), later)
    count = lax.axis_size(TILE)
    far = lax.ppermute(far, TILE, [(t, (t - 1 + 2 * (t % 2)) % count) for t in range(count)])
    near = lax.ppermute(near, TILE, [(t, t + 1 - 2 * (t % 2)) for t in range(count)])
    ns = vertical(ns)
    return (partner, ns, near, far), later


def share(stat):
    copies = stat.reshape(DEVICES, 1, LANES)
    return lax.all_to_all(copies, TILE_SPLIT, 0, 0).reshape(DEVICES, LANES)


def meet(scalars, pack, stat, width):
    received = exchange(scalars, pack, width)[0] if pack is not None else None
    return (share(stat) if stat is not None else None), received


def embedding(timestep, time_weight, bias_upper, bias_lower):
    moment = timestep[0].astype(F32)
    half_width = time_weight.shape[0] // 2
    frequencies = jnp.exp(-math.log(10000.0) * jnp.arange(half_width, dtype=F32) / half_width)
    angles = moment * frequencies
    features = jnp.concatenate([jnp.sin(angles), jnp.cos(angles)])[None, :]
    embedded = jax.nn.silu(jnp.dot(features, time_weight, precision=lax.Precision.HIGHEST))
    both = jnp.concatenate([bias_upper, bias_lower], axis=1)
    biases = jnp.dot(embedded, both, precision=lax.Precision.HIGHEST)
    return biases


def flat_kernel(kernel):
    return jnp.transpose(kernel, (2, 0, 1, 3)).reshape(kernel.shape[2], -1)


def deep_kernel(kernel):
    wide = kernel.astype(F32)
    none = jnp.zeros_like(wide[0])
    even = jnp.stack([wide[0], wide[1] + wide[2], none])
    odd = jnp.stack([none, wide[0] + wide[1], wide[2]])
    both = jnp.stack([even, odd]).astype(BF16)
    return jnp.transpose(both, (0, 3, 1, 2, 4)).reshape(2 * kernel.shape[2], -1)


def per_device(
    noisy_image,
    seam_codes,
    timestep,
    time_weight,
    bias_upper,
    bias_lower,
    kernel_upper_first,
    kernel_upper_second,
    kernel_lower_first,
    kernel_lower_second,
    kernel_decode_first,
    kernel_decode_second,
    output_weight,
    gains_upper,
    shifts_upper,
    gains_lower,
    shifts_lower,
):
    here = jnp.stack([lax.axis_index(TILE), lax.axis_index("split")]).astype(jnp.int32)
    channels, block_rows, width = noisy_image.shape[1:]
    padding = kernel_upper_first.shape[2] - channels
    image = jnp.transpose(jnp.pad(noisy_image[0], ((0, padding), (0, 0), (0, 0))), (1, 0, 2))
    low_width = width // 2
    width_one = kernel_upper_first.shape[2]

    pack = edges_of_image(here, image)
    scalars = setup(here, seam_codes.T)
    early = (timestep, time_weight, bias_upper, bias_lower, kernel_upper_first, kernel_upper_second)
    late = (kernel_lower_first, kernel_lower_second, kernel_decode_first, kernel_decode_second, output_weight)
    received, early = exchange(scalars, pack, width, early)
    params = one_table(scalars, (gains_upper, shifts_upper, gains_lower, shifts_lower))
    timestep, time_weight, bias_upper, bias_lower, kernel_upper_first, kernel_upper_second = early
    biases = embedding(timestep, time_weight, bias_upper, bias_lower)
    weights = (
        flat_kernel(jnp.pad(kernel_upper_first, ((0, 0), (0, 0), (0, 0), (0, padding)))),
        flat_kernel(kernel_upper_second),
        biases,
    )
    received, (upper_first, upper_second, biases) = lax.optimization_barrier((received, weights))
    raw, pack, stat = first_stage(scalars, image, *received, upper_first, biases)

    received, late = exchange(scalars, pack, width, late)
    stats = share(stat)
    kernel_lower_first, kernel_lower_second, kernel_decode_first, kernel_decode_second, output_weight = late
    weights = (
        flat_kernel(kernel_lower_first),
        flat_kernel(kernel_lower_second),
        flat_kernel(kernel_decode_first[..., -width_one:]),
        deep_kernel(kernel_decode_first[..., :-width_one]),
        flat_kernel(kernel_decode_second),
        jnp.pad(output_weight, ((0, padding), (0, 0))),
    )
    received, weights = lax.optimization_barrier((received, weights))
    lower_first, lower_second, decode_skip, decode_deep, decode_second, project = weights
    stats = coef_stage(scalars, stats, params, 0, biases, 0, width_one, block_rows * width)
    raw, stat, pack = plain_stage(scalars, raw, stats, *received, upper_second, params, biases, width, 2)

    stats, received = meet(scalars, pack, stat, width)
    stats = coef_stage(scalars, stats, params, 1, None, 0, width_one, block_rows * width)
    skip, sides, raw, pack, stat = pool_stage(
        scalars, raw, stats, *received, lower_first, params, biases
    )

    stats, received = meet(scalars, pack, stat, low_width)
    part = skip_stage(scalars, skip, sides, decode_skip)
    stats = coef_stage(scalars, stats, params, 8, biases, width_one, 2 * width_one, block_rows * width // 4)
    raw, stat, pack = plain_stage(
        scalars, raw, stats, *received, lower_second, params, biases,
        low_width, 1,
    )

    stats, received = meet(scalars, pack, stat, low_width)
    stats = coef_stage(scalars, stats, params, 9, None, 0, 2 * width_one, block_rows * width // 4)
    raw, pack, stat = decode_stage(
        scalars, raw, stats, *received, part, decode_deep, params
    )

    stats, received = meet(scalars, pack, stat, width)
    stats = coef_stage(scalars, stats, params, 2, None, 0, width_one, block_rows * width)
    raw, stat = plain_stage(scalars, raw, stats, *received, decode_second, params, None, width, 0)

    stats, _ = meet(scalars, None, stat, width)
    result = project_stage(scalars, raw, stats, project, params, channels)
    return jnp.transpose(result, (1, 0, 2))[None]


def solution(mesh):
    torus = Mesh(
        mesh.devices.reshape(4, 4, 2, 2, mesh.shape["split"]),
        ("tile_0", "tile_1", "tile_2", "tile_3", "split"),
    )
    return jax.shard_map(
        per_device,
        mesh=torus,
        in_specs=(P(TILE, None, "split", None),) + (P(),) * 16,
        out_specs=P(TILE, None, "split", None),
        check_vma=False,
    )
```
